128 devices in a mesh: shot: 8 (over y, core), rcv: 16 (over z, x).
Axes of the slice: x: 4, y: 4, z: 4, core: 2. Of those that a mesh axis runs over, the one named last changes fastest.
Arguments:
- traces: bfloat16 [8, 16, 1536, 2048], P('shot', 'rcv'), may hold values from -6 to 6
- trace_shot: int32 [8, 16, 1536], P('shot', 'rcv'), may hold values from 0 to 127, as said below
- trace_rcv: int32 [8, 16, 1536], P('shot', 'rcv'), may hold values from 0 to 127
- fold_count: int32 [8, 16], P('shot', 'rcv'), may hold values from 512 to 1536
Outputs:
- shot_terms: float32 [1024, 1024], P('shot')
- rcv_terms: float32 [2048, 1024], P('rcv')
The draws below stay inside these ranges and needn't reach their ends.
Inputs may be any that keep to these rules, and one draw needn't show every extreme that they name: `trace_shot`: in every tile, slot k < 128 holds a distinct shot, and its receiver index equals its shot index, so every shot and receiver of the tile's blocks has a live trace there.
All inputs are finite; a program needn't handle non-finite values.
Results may differ from the reference program's by a relative error of at most 0.0072.
Values sent between devices are 32-bit elements; how exact they have to be, the bound alone decides.
A program may use at most 128 MiB of HBM per device.

```python
import jax
import jax.numpy as jnp
from jax import lax

SAMPLES = 2048
FREQS = 1024
SHOT_DEV = 128
RCV_DEV = 128
TRACE_DEV = 1536
SWEEPS = 3
N_SHOT = 8
N_RCV = 16


def slot_layout(key):
    base_key = jax.random.fold_in(key, 7)
    slots = jnp.arange(TRACE_DEV, dtype=jnp.int32)[None, None, :]
    shifts = jax.random.randint(jax.random.fold_in(base_key, 1), (N_SHOT, N_RCV, 1), 0, SHOT_DEV)
    random_shot = jax.random.randint(jax.random.fold_in(base_key, 2), (N_SHOT, N_RCV, TRACE_DEV), 0, SHOT_DEV)
    offsets = jax.random.randint(jax.random.fold_in(base_key, 3), (N_SHOT, N_RCV, TRACE_DEV), -4, 5)
    first_rows = slots < SHOT_DEV
    shot_index = jnp.where(first_rows, (slots + shifts) % SHOT_DEV, random_shot)
    offsets = jnp.where(first_rows, 0, offsets)
    rcv_index = (shot_index + offsets + RCV_DEV) % RCV_DEV
    return (shot_index.astype(jnp.int32), rcv_index.astype(jnp.int32))


def draw_trace_shot(key, part):
    return slot_layout(key)[0]


def draw_trace_rcv(key, part):
    return slot_layout(key)[1]


def draw_fold_count(key, part):
    count_key = jax.random.fold_in(key, 11)
    return jax.random.randint(count_key, (N_SHOT, N_RCV), TRACE_DEV // 3, TRACE_DEV + 1).astype(jnp.int32)


def levels(own_key, dims, split, low, top_value):
    gain = 1.0
    for axis_at, parts in split:
        draws = jax.random.uniform(jax.random.fold_in(jax.random.fold_in(own_key, 6), axis_at), (parts,), jnp.float32, low / len(split), top_value / len(split))
        gain = gain * jnp.repeat(jnp.exp(draws), dims[axis_at] // parts).reshape((-1,) + (1,) * (len(dims) - 1 - axis_at))
    return gain


def scatter_about(stream_key, extent, spread, most, shards=(), held_as=jnp.bfloat16):
    array = spread * jax.random.normal(stream_key, extent, jnp.float32)
    if shards:
        array = array * levels(stream_key, extent, shards, -0.22, 0.18)
    return jnp.clip(array, -most, most).astype(held_as)


def setup_inputs(seed: int = 0) -> dict:
    streams_of = jax.random.split(jax.random.key(seed), 5)
    traces = scatter_about(streams_of[0], (N_SHOT, N_RCV, TRACE_DEV, SAMPLES), 1.0, 6.0, ((0, 8), (1, 16)))
    trace_shot = draw_trace_shot(jax.random.fold_in(streams_of[4], 71), 0)
    trace_rcv = draw_trace_rcv(jax.random.fold_in(streams_of[4], 71), 0)
    fold_count = draw_fold_count(jax.random.fold_in(streams_of[4], 71), 0)
    return dict(traces=traces, trace_shot=trace_shot, trace_rcv=trace_rcv, fold_count=fold_count)


def dft_tables():
    index_n = jnp.arange(SAMPLES, dtype=jnp.int32)
    index_f = jnp.arange(FREQS, dtype=jnp.int32)
    product = (index_n[:, None] * index_f[None, :]) % SAMPLES
    angle_table = (2.0 * jnp.pi / SAMPLES) * product.astype(jnp.float32)
    return jnp.cos(angle_table).astype(jnp.bfloat16), jnp.sin(angle_table).astype(jnp.bfloat16)


def reference(traces, trace_shot, trace_rcv, fold_count):
    cos_table, sin_table = dft_tables()
    tiles_total = N_SHOT * N_RCV
    flat_traces = traces.reshape(tiles_total, TRACE_DEV, SAMPLES)
    flat_shot = trace_shot.reshape(tiles_total, TRACE_DEV)
    flat_rcv = trace_rcv.reshape(tiles_total, TRACE_DEV)
    flat_count = fold_count.reshape(tiles_total)

    def tile_sums(packed):
        tile_traces, tile_shot, tile_rcv, tile_count = packed
        real = jnp.dot(tile_traces, cos_table, preferred_element_type=jnp.float32)
        imag = jnp.dot(tile_traces, sin_table, preferred_element_type=jnp.float32)
        log_power = jnp.log((real * real + imag * imag) / SAMPLES + 1e-6)
        alive = (jnp.arange(TRACE_DEV, dtype=jnp.int32) < tile_count).astype(log_power.dtype)
        onehot_shot = (tile_shot[:, None] == jnp.arange(SHOT_DEV, dtype=jnp.int32)[None, :]).astype(log_power.dtype) * alive[:, None]
        onehot_rcv = (tile_rcv[:, None] == jnp.arange(RCV_DEV, dtype=jnp.int32)[None, :]).astype(log_power.dtype) * alive[:, None]
        shot_logs = jnp.dot(onehot_shot.T, log_power, precision=lax.Precision.HIGHEST)
        rcv_logs = jnp.dot(onehot_rcv.T, log_power, precision=lax.Precision.HIGHEST)
        pairs = jnp.dot(onehot_shot.T, onehot_rcv, precision=lax.Precision.HIGHEST)
        return shot_logs, rcv_logs, pairs

    shot_logs, rcv_logs, pairs = lax.map(tile_sums, (flat_traces, flat_shot, flat_rcv, flat_count))
    shot_logs = shot_logs.reshape(N_SHOT, N_RCV, SHOT_DEV, FREQS).sum(axis=1)
    rcv_logs = rcv_logs.reshape(N_SHOT, N_RCV, RCV_DEV, FREQS).sum(axis=0)
    pairs = pairs.reshape(N_SHOT, N_RCV, SHOT_DEV, RCV_DEV)
    shot_count = pairs.sum(axis=3).sum(axis=1)
    rcv_count = pairs.sum(axis=2).sum(axis=0)
    rcv_terms = jnp.zeros((N_RCV, RCV_DEV, FREQS), shot_logs.dtype)
    shot_terms = jnp.zeros((N_SHOT, SHOT_DEV, FREQS), shot_logs.dtype)
    for iteration in range(SWEEPS):
        shot_total = shot_logs - jnp.einsum("ijxy,jyf->ixf", pairs, rcv_terms, precision=lax.Precision.HIGHEST)
        shot_terms = shot_total / shot_count[:, :, None]
        rcv_total = rcv_logs - jnp.einsum("ijxy,ixf->jyf", pairs, shot_terms, precision=lax.Precision.HIGHEST)
        rcv_terms = rcv_total / rcv_count[:, :, None]
    return shot_terms.reshape(N_SHOT * SHOT_DEV, FREQS), rcv_terms.reshape(N_RCV * RCV_DEV, FREQS)
```

```python
import functools
import math

import jax
import jax.numpy as jnp
import numpy as np
from jax import lax
from jax.experimental import pallas as pl
from jax.experimental.pallas import tpu as pltpu
from jax.sharding import PartitionSpec as P

MESH = pl.DeviceIdType.MESH
VMEM = pltpu.VMEM
SWEEPS = 3
LANES = 128
CHIPS = 64
PLANE = 16
RINGS = 4
OWNED = 16
NT = (((1,), (1,)), ((), ()))
VMEM_LIMIT = 60 * 1024 * 1024


def phase_tables(samples):
    lane = np.arange(LANES)
    tile = np.arange(LANES)
    rows, turns = [], []
    for odd in range(2):
        angle = 2 * np.pi * ((8 * tile[:, None] * (2 * lane[None, :] + odd)) % samples) / samples
        rows.append(np.stack([np.cos(angle), np.sin(angle)]))
    sub = np.arange(8)
    for odd in range(2):
        for q in range(4):
            freq = 256 * q + 2 * lane + odd
            angle = 2 * np.pi * ((sub[:, None] * freq[None, :]) % samples) / samples
            turns.append(np.stack([np.cos(angle), np.sin(angle)]))
    return np.stack(rows).astype(np.float32), np.stack(turns).astype(np.float32)


def fill_table(table, rows_ref, turns_ref, odd, chunk):
    turn_c, turn_s = turns_ref[chunk, 0], turns_ref[chunk, 1]

    def step(m, carry):
        cos_rows, sin_rows = [], []
        for half in range(2):
            at = 2 * m + half
            rc = jnp.broadcast_to(rows_ref[odd, 0, pl.ds(at, 1), :], (8, LANES))
            rs = jnp.broadcast_to(rows_ref[odd, 1, pl.ds(at, 1), :], (8, LANES))
            cos_rows.append(rc * turn_c - rs * turn_s)
            sin_rows.append(rs * turn_c + rc * turn_s)
        at = pl.ds(pl.multiple_of(m * 16, 16), 16)
        table[at, :LANES] = jnp.concatenate(cos_rows, axis=0).astype(jnp.bfloat16)
        table[at, LANES:] = jnp.concatenate(sin_rows, axis=0).astype(jnp.bfloat16)
        return carry

    lax.fori_loop(0, 64, step, 0, unroll=8)


def one_hot(row, ids):
    wide = jnp.broadcast_to(row, (16, LANES)).astype(jnp.bfloat16)
    wide = jnp.concatenate([wide] * 8, axis=0)
    return jnp.where(wide == ids, jnp.ones_like(ids), jnp.zeros_like(ids))


def sublane_ids():
    return lax.broadcasted_iota(jnp.int32, (LANES, LANES), 0).astype(jnp.float32).astype(jnp.bfloat16)


def spectra_kernel(traces, index, rows_ref, turns_ref, out, held, folded, table, hot, sums, sem):
    slots, samples = held.shape
    half = samples // 2
    block = 256
    copies = []
    for b in range(slots // block):
        at = pl.ds(b * block, block)
        copy = pltpu.make_async_copy(traces.at[at], held.at[at], sem.at[b])
        copy.start()
        copies.append(copy)
    ids = sublane_ids()
    values = index[...].astype(jnp.float32)
    tiles = slots // LANES
    for r in range(tiles):
        hot[:LANES, r * LANES : (r + 1) * LANES] = one_hot(values[r : r + 1], ids)
        hot[LANES:, r * LANES : (r + 1) * LANES] = one_hot(values[tiles + r : tiles + r + 1], ids)
    for b, copy in enumerate(copies):
        copy.wait()
        at = pl.ds(b * block, block)
        low, high = held[at, :half].astype(jnp.float32), held[at, half:].astype(jnp.float32)
        folded[0, at, :] = (low + high).astype(jnp.bfloat16)
        folded[1, at, :] = (low - high).astype(jnp.bfloat16)

    def chunk_step(chunk, carry):
        odd = chunk // 4
        fill_table(table, rows_ref, turns_ref, odd, chunk)
        sums[...] = jnp.zeros_like(sums)
        for b in range(slots // 512):
            at = pl.ds(b * 512, 512)
            both = jnp.dot(folded[odd, at, :], table[...], preferred_element_type=jnp.float32)
            real, imag = both[:, :LANES], both[:, LANES:]
            logs = jnp.log((real * real + imag * imag) * (1.0 / samples) + 1e-6)
            top = logs.astype(jnp.bfloat16)
            rest = (logs - top.astype(jnp.float32)).astype(jnp.bfloat16)
            sums[...] += jnp.dot(
                hot[:, b * 512 : (b + 1) * 512],
                jnp.concatenate([top, rest], axis=1),
                preferred_element_type=jnp.float32,
            )
        total = (sums[:, :LANES] + sums[:, LANES:]).T
        at = pl.ds(chunk * 8, 8)
        out[at, :OWNED, :] = total[:, :LANES].reshape(8, OWNED, LANES)
        out[at, OWNED:, :] = total[:, LANES:].reshape(8, OWNED, LANES)
        return carry

    lax.fori_loop(0, 8, chunk_step, 0)


def my_place():
    shot, rcv = lax.axis_index("shot"), lax.axis_index("rcv")
    return shot // 2, lax.rem(shot, 2), rcv // 4, lax.rem(rcv, 4)


def other(k, place):
    y, core, z, x = place
    ty = lax.rem(y + k // 16, 4)
    tz = lax.rem(z + lax.rem(k // 4, 4), 4)
    tx = lax.rem(x + lax.rem(k, 4), 4)
    rcv = tz * 4 + tx
    return ty, rcv, ty * PLANE + rcv, (ty * 2 + core, rcv)


def greet(place, partner):
    barrier = pltpu.get_barrier_semaphore()

    def step(k, carry):
        pl.semaphore_signal(barrier, inc=1, device_id=other(k, place)[3], device_id_type=MESH)
        return carry

    lax.fori_loop(1, CHIPS, step, 0)
    if partner is not None:
        pl.semaphore_signal(barrier, inc=1, device_id=partner, device_id_type=MESH)
    pl.semaphore_wait(barrier, CHIPS - 1 + (partner is not None))


def exchange_kernel(index, blocks, index_all, shot_out, rcv_out, landed, index_landed, sems):
    place = my_place()
    y, core, z, x = place
    me = y * PLANE + z * 4 + x
    greet(place, None)

    def copies(k):
        ty, rcv, number, device = other(k, place)
        a = pltpu.make_async_remote_copy(
            index, index_landed.at[me], sems.at[0, number], sems.at[1, me], device_id=device, device_id_type=MESH
        )
        b = pltpu.make_async_remote_copy(
            blocks.at[number], landed.at[me], sems.at[2, number], sems.at[3, me], device_id=device, device_id_type=MESH
        )
        return a, b

    def arrivals(k):
        ty, rcv, number, device = other(k, place)
        a = pltpu.make_async_remote_copy(
            index, index_landed.at[number], sems.at[0, number], sems.at[1, number], device_id=device, device_id_type=MESH
        )
        b = pltpu.make_async_remote_copy(
            blocks.at[number], landed.at[number], sems.at[2, number], sems.at[3, number], device_id=device, device_id_type=MESH
        )
        return a, b

    def start(k, carry):
        for copy in copies(k):
            copy.start()
        return carry

    lax.fori_loop(1, CHIPS, start, 0)
    landed[me] = blocks[me]
    index_landed[me] = index[...]

    def finish(k, carry):
        for copy in arrivals(k):
            copy.wait()
        return carry

    lax.fori_loop(1, CHIPS, finish, 0)
    index_all[...] = index_landed[...]
    for b in range(RINGS):
        shot_out[:, b * LANES : (b + 1) * LANES] = landed[b * PLANE : (b + 1) * PLANE, :OWNED, :].sum(axis=0)
    whole = landed[:PLANE, OWNED:, :]
    for b in range(1, RINGS):
        whole = whole + landed[b * PLANE : (b + 1) * PLANE, OWNED:, :]
    for j in range(PLANE):
        rcv_out[:, j * LANES : (j + 1) * LANES] = whole[j]


def pairs_kernel(index_all, pairs, shot_count, rcv_count, hot, totals):
    tiles = index_all.shape[1] // 2
    ids = sublane_ids()
    totals[...] = jnp.zeros_like(totals)
    rcv_count[...] = jnp.zeros_like(rcv_count)

    def step(p, carry):
        block, j = p // PLANE, lax.rem(p, PLANE)
        values = index_all[p].astype(jnp.float32)
        shots = jnp.concatenate([one_hot(values[r : r + 1], ids) for r in range(tiles)], axis=1)
        rcvs = jnp.concatenate([one_hot(values[tiles + r : tiles + r + 1], ids) for r in range(tiles)], axis=1)
        pair = lax.dot_general(shots, rcvs, NT, preferred_element_type=jnp.float32)
        across = pl.ds(pl.multiple_of(j * LANES, LANES), LANES)
        pairs[pl.ds(pl.multiple_of(block * LANES, LANES), LANES), across] = pair.astype(jnp.bfloat16)
        totals[block] += pair
        rcv_count[:, across] += jnp.broadcast_to(pair.sum(axis=0, keepdims=True), (8, LANES))
        return carry

    lax.fori_loop(0, CHIPS, step, 0, unroll=2)
    for b in range(RINGS):
        row = totals[b].T.sum(axis=0, keepdims=True)
        shot_count[:, b * LANES : (b + 1) * LANES] = jnp.broadcast_to(row, (8, LANES))


def two_parts(value):
    top = value.astype(jnp.bfloat16)
    return jnp.concatenate([top, (value - top.astype(jnp.float32)).astype(jnp.bfloat16)], axis=0)


def sweeps_kernel(shot_logs, rcv_logs, pairs, shot_count, rcv_count, shot_out, rcv_out,
                  shot_send, rcv_send, shot_land, rcv_land, count_land, part_send, part_land, sems, part_sems):
    place = my_place()
    y, core, z, x = place
    me = y * PLANE + z * 4 + x
    partner = (y * 2 + 1 - core, z * 4 + x)
    greet(place, partner)

    def pair_copy(src, dst, n):
        return pltpu.make_async_remote_copy(
            src, dst, part_sems.at[0, n], part_sems.at[1, n], device_id=partner, device_id_type=MESH
        )

    count_copy = pair_copy(rcv_count, count_land, SWEEPS)
    count_copy.start()
    counts = shot_count[0:1, :]
    rcv_counts = None
    rcv_terms = None
    copies = [pair_copy(part_send.at[n], part_land.at[n], n) for n in range(SWEEPS)]

    def copy_to(src, dst, kind, k, mine):
        ty, rcv, number, device = other(k, place)
        at = me if mine else number
        source = src.at[ty] if kind == 0 else src.at[rcv]
        return pltpu.make_async_remote_copy(
            source, dst.at[at], sems.at[2 * kind, number], sems.at[2 * kind + 1, at], device_id=device, device_id_type=MESH
        )

    def send_all(src, dst, kind):
        def step(k, carry):
            copy_to(src, dst, kind, k, True).start()
            return carry

        lax.fori_loop(1, CHIPS, step, 0)

    for n in range(SWEEPS):
        if n == 0:
            shot_terms = shot_logs[...] / counts
        else:
            both = lax.dot_general(two_parts(rcv_terms), pairs[...], NT, preferred_element_type=jnp.float32)
            shot_terms = (shot_logs[...] - (both[:OWNED] + both[OWNED:])) / counts
        if n == SWEEPS - 1:
            for b in range(RINGS):
                shot_send[b] = shot_terms[:, b * LANES : (b + 1) * LANES]
            send_all(shot_send, shot_land, 0)
        both = jnp.dot(two_parts(shot_terms), pairs[...], preferred_element_type=jnp.float32)
        part = rcv_logs[...] - (both[:OWNED] + both[OWNED:])
        part_send[n] = part
        copies[n].start()
        if n == 0:
            count_copy.wait()
            rcv_counts = rcv_count[0:1, :] + count_land[0:1, :]
        copies[n].wait()
        rcv_terms = (part + part_land[n]) / rcv_counts
    for j in range(PLANE):
        rcv_send[j] = rcv_terms[:, j * LANES : (j + 1) * LANES]
    send_all(rcv_send, rcv_land, 1)
    shot_land[me] = shot_send[y]
    rcv_land[me] = rcv_send[z * 4 + x]

    def finish(k, carry):
        copy_to(shot_send, shot_land, 0, k, False).wait()
        copy_to(rcv_send, rcv_land, 1, k, False).wait()
        return carry

    lax.fori_loop(1, CHIPS, finish, 0)
    shot_out[...] = shot_land[...]
    rcv_out[...] = rcv_land[...]


def turn_kernel(shot_in, rcv_in, shot_out, rcv_out, order):
    half = order.shape[0] // 2
    for src, dst in ((shot_in, shot_out), (rcv_in, rcv_out)):
        order[pl.ds(0, half, stride=2), :] = src[:half]
        order[pl.ds(1, half, stride=2), :] = src[half:]
        dst[...] = order[...].T


def shards(traces, trace_shot, trace_rcv, fold_count):
    slots, samples = traces.shape[2:]
    bins = samples // 2
    tiles = slots // LANES
    rows_np, turns_np = phase_tables(samples)
    alive = jnp.arange(slots, dtype=jnp.int32).reshape(1, tiles, LANES) < fold_count[0, 0]
    index = jnp.stack([trace_shot[0, 0], trace_rcv[0, 0]]).reshape(2, tiles, LANES)
    index = jnp.where(alive, index, -1).reshape(2 * tiles, LANES)
    f32, bf16 = jnp.float32, jnp.bfloat16
    vmem = pl.BlockSpec(memory_space=VMEM)
    shape = jax.ShapeDtypeStruct
    blocks = pl.pallas_call(
        spectra_kernel,
        out_shape=shape((CHIPS, 2 * OWNED, LANES), f32),
        in_specs=[pl.BlockSpec(memory_space=pl.ANY), vmem, vmem, vmem],
        out_specs=vmem,
        scratch_shapes=[
            VMEM((slots, samples), bf16),
            VMEM((2, slots, samples // 2), bf16),
            VMEM((samples // 2, 2 * LANES), bf16),
            VMEM((2 * LANES, slots), bf16),
            VMEM((2 * LANES, 2 * LANES), f32),
            pltpu.SemaphoreType.DMA((slots // 256,)),
        ],
        compiler_params=pltpu.CompilerParams(vmem_limit_bytes=VMEM_LIMIT),
        name="spectra",
    )(traces[0, 0], index, jnp.asarray(rows_np), jnp.asarray(turns_np))
    index_all, shot_logs, rcv_logs = pl.pallas_call(
        exchange_kernel,
        out_shape=(
            shape((CHIPS, 2 * tiles, LANES), jnp.int32),
            shape((OWNED, RINGS * LANES), f32),
            shape((OWNED, PLANE * LANES), f32),
        ),
        in_specs=[vmem, vmem],
        out_specs=(vmem,) * 3,
        scratch_shapes=[
            VMEM((CHIPS, 2 * OWNED, LANES), f32),
            VMEM((CHIPS, 2 * tiles, LANES), jnp.int32),
            pltpu.SemaphoreType.DMA((4, CHIPS)),
        ],
        compiler_params=pltpu.CompilerParams(
            collective_id=0, has_side_effects=True, vmem_limit_bytes=VMEM_LIMIT
        ),
        name="exchange",
    )(index, blocks)
    pairs, shot_count, rcv_count = pl.pallas_call(
        pairs_kernel,
        out_shape=(
            shape((RINGS * LANES, PLANE * LANES), bf16),
            shape((8, RINGS * LANES), f32),
            shape((8, PLANE * LANES), f32),
        ),
        in_specs=[vmem],
        out_specs=(vmem,) * 3,
        scratch_shapes=[VMEM((8, LANES), f32), VMEM((RINGS, LANES, LANES), f32)],
        compiler_params=pltpu.CompilerParams(vmem_limit_bytes=VMEM_LIMIT),
        name="pairs",
    )(index_all)
    shot_got, rcv_got = pl.pallas_call(
        sweeps_kernel,
        out_shape=(shape((CHIPS, OWNED, LANES), f32), shape((CHIPS, OWNED, LANES), f32)),
        in_specs=[vmem] * 5,
        out_specs=(vmem,) * 2,
        scratch_shapes=[
            VMEM((RINGS, OWNED, LANES), f32),
            VMEM((PLANE, OWNED, LANES), f32),
            VMEM((CHIPS, OWNED, LANES), f32),
            VMEM((CHIPS, OWNED, LANES), f32),
            VMEM((8, PLANE * LANES), f32),
            VMEM((SWEEPS, OWNED, PLANE * LANES), f32),
            VMEM((SWEEPS, OWNED, PLANE * LANES), f32),
            pltpu.SemaphoreType.DMA((4, CHIPS)),
            pltpu.SemaphoreType.DMA((2, SWEEPS + 1)),
        ],
        compiler_params=pltpu.CompilerParams(
            collective_id=1, has_side_effects=True, vmem_limit_bytes=VMEM_LIMIT
        ),
        name="sweeps",
    )(shot_logs, rcv_logs, pairs, shot_count, rcv_count)
    return pl.pallas_call(
        turn_kernel,
        out_shape=(shape((LANES, bins), f32), shape((LANES, bins), f32)),
        in_specs=[vmem] * 2,
        out_specs=(vmem,) * 2,
        scratch_shapes=[VMEM((bins, LANES), f32)],
        compiler_params=pltpu.CompilerParams(vmem_limit_bytes=VMEM_LIMIT),
        name="turn",
    )(shot_got.reshape(bins, LANES), rcv_got.reshape(bins, LANES))


def solution(mesh):
    return jax.shard_map(
        shards,
        mesh=mesh,
        in_specs=(
            P("shot", "rcv", None, None),
            P("shot", "rcv", None),
            P("shot", "rcv", None),
            P("shot", "rcv"),
        ),
        out_specs=(P("shot", None), P("rcv", None)),
        check_vma=False,
    )
```

```python
import functools
import math

import jax
import jax.numpy as jnp
import numpy as np
from jax import lax
from jax.experimental import pallas as pl
from jax.experimental.pallas import tpu as pltpu
from jax.sharding import PartitionSpec as P

MESH = pl.DeviceIdType.MESH
VMEM = pltpu.VMEM
SWEEPS = 3
LANES = 128
CHIPS = 64
PLANE = 16
RINGS = 4
OWNED = 16
NT = (((1,), (1,)), ((), ()))
VMEM_LIMIT = 60 * 1024 * 1024


def phase_tables(samples):
    lane = np.arange(LANES)
    tile = np.arange(LANES)
    rows, turns = [], []
    for odd in range(2):
        angle = 2 * np.pi * ((8 * tile[:, None] * (2 * lane[None, :] + odd)) % samples) / samples
        rows.append(np.stack([np.cos(angle), np.sin(angle)]))
    sub = np.arange(8)
    for odd in range(2):
        for q in range(4):
            freq = 256 * q + 2 * lane + odd
            angle = 2 * np.pi * ((sub[:, None] * freq[None, :]) % samples) / samples
            turns.append(np.stack([np.cos(angle), np.sin(angle)]))
    return np.stack(rows).astype(np.float32), np.stack(turns).astype(np.float32)


def fill_table(table, rows_ref, turns_ref, odd, chunk):
    turn_c, turn_s = turns_ref[chunk, 0], turns_ref[chunk, 1]
    half = table.shape[0] // 2
    sign = (1 - 2 * odd).astype(jnp.float32)

    def step(m, carry):
        cos_rows, sin_rows = [], []
        for part in range(2):
            at = 2 * m + part
            rc = jnp.broadcast_to(rows_ref[odd, 0, pl.ds(at, 1), :], (8, LANES))
            rs = jnp.broadcast_to(rows_ref[odd, 1, pl.ds(at, 1), :], (8, LANES))
            cos_rows.append(rc * turn_c - rs * turn_s)
            sin_rows.append(rs * turn_c + rc * turn_s)
        both = jnp.concatenate([jnp.concatenate(cos_rows, axis=0), jnp.concatenate(sin_rows, axis=0)], axis=1)
        start = pl.multiple_of(m * 16, 16)
        table[pl.ds(start, 16), :] = both.astype(jnp.bfloat16)
        table[pl.ds(start + half, 16), :] = (both * sign).astype(jnp.bfloat16)
        return carry

    lax.fori_loop(0, 64, step, 0, unroll=8)


def one_hot(row, ids):
    wide = jnp.broadcast_to(row, (16, LANES)).astype(jnp.bfloat16)
    wide = jnp.concatenate([wide] * 8, axis=0)
    return jnp.where(wide == ids, jnp.ones_like(ids), jnp.zeros_like(ids))


def sublane_ids():
    return lax.broadcasted_iota(jnp.int32, (LANES, LANES), 0).astype(jnp.float32).astype(jnp.bfloat16)


def my_place():
    shot, rcv = lax.axis_index("shot"), lax.axis_index("rcv")
    return shot // 2, lax.rem(shot, 2), rcv // 4, lax.rem(rcv, 4)


def other(k, place):
    y, core, z, x = place
    ty = lax.rem(y + k // 16, 4)
    tz = lax.rem(z + lax.rem(k // 4, 4), 4)
    tx = lax.rem(x + lax.rem(k, 4), 4)
    rcv = tz * 4 + tx
    return ty, rcv, ty * PLANE + rcv, (ty * 2 + core, rcv)


def device_of(number, core):
    return (number // PLANE) * 2 + core, lax.rem(number, PLANE)


def greet(place, partner):
    barrier = pltpu.get_barrier_semaphore()

    def step(k, carry):
        pl.semaphore_signal(barrier, inc=1, device_id=other(k, place)[3], device_id_type=MESH)
        return carry

    lax.fori_loop(1, CHIPS, step, 0)
    pl.semaphore_signal(barrier, inc=1, device_id=partner, device_id_type=MESH)
    return lambda: pl.semaphore_wait(barrier, CHIPS)


def two_parts(value, axis):
    top = value.astype(jnp.bfloat16)
    return jnp.concatenate([top, (value - top.astype(jnp.float32)).astype(jnp.bfloat16)], axis=axis)


def main_kernel(traces, index, rows_ref, turns_ref, shot_out, rcv_out,
                held, table, hot, blocks, landed, index_landed,
                pairs, totals, rcv_count, count_land,
                shot_send, rcv_send, shot_land, rcv_land, part_send, part_land,
                trace_sem, sems, term_sems, part_sems):
    place = my_place()
    y, core, z, x = place
    mine = z * 4 + x
    me = y * PLANE + mine
    partner = (y * 2 + 1 - core, mine)
    slots, samples = held.shape
    tiles = slots // LANES

    all_here = greet(place, partner)
    block = 512
    loads = [
        pltpu.make_async_copy(traces.at[pl.ds(b * block, block)], held.at[pl.ds(b * block, block)], trace_sem.at[b])
        for b in range(slots // block)
    ]
    for load in loads:
        load.start()
    ids = sublane_ids()
    values = index[...].astype(jnp.float32)
    for r in range(tiles):
        hot[:LANES, r * LANES : (r + 1) * LANES] = one_hot(values[r : r + 1], ids)
        hot[LANES:, r * LANES : (r + 1) * LANES] = one_hot(values[tiles + r : tiles + r + 1], ids)
    index_landed[me] = index[...]
    all_here()

    def index_copy(k, slot):
        number, device = other(k, place)[2:]
        return pltpu.make_async_remote_copy(
            index, index_landed.at[number if slot is None else slot], sems.at[0, number],
            sems.at[1, number if slot is None else slot], device_id=device, device_id_type=MESH
        )

    def block_copy(number, slot):
        return pltpu.make_async_remote_copy(
            blocks.at[number], landed.at[slot], sems.at[2, number], sems.at[3, slot],
            device_id=device_of(number, core), device_id_type=MESH
        )

    def send_index(k, carry):
        index_copy(k, me).start()
        return carry

    lax.fori_loop(1, CHIPS, send_index, 0)
    for load in loads:
        load.wait()

    def chunk_step(t, carry):
        chunk = lax.rem(t + me, 8)
        fill_table(table, rows_ref, turns_ref, chunk // 4, chunk)
        total = None
        for b in range(slots // block):
            both = jnp.dot(held[b * block : (b + 1) * block], table[...], preferred_element_type=jnp.float32)
            real, imag = both[:, :LANES], both[:, LANES:]
            logs = jnp.log((real * real + imag * imag) * (1.0 / samples) + 1e-6)
            part = jnp.dot(
                hot[:, b * block : (b + 1) * block], two_parts(logs, 1), preferred_element_type=jnp.float32
            )
            total = part if total is None else total + part
        total = (total[:, :LANES] + total[:, LANES:]).T
        at = pl.ds(chunk * 8, 8)
        blocks[at, :OWNED, :] = total[:, :LANES].reshape(8, OWNED, LANES)
        blocks[at, OWNED:, :] = total[:, LANES:].reshape(8, OWNED, LANES)

        def send(n, inner):
            number = chunk * 8 + n

            @pl.when(number != me)
            def _():
                block_copy(number, me).start()

            return inner

        lax.fori_loop(0, 8, send, 0)
        return carry

    lax.fori_loop(0, 8, chunk_step, 0)
    landed[me] = blocks[me]

    totals[...] = jnp.zeros_like(totals)
    rcv_count[...] = jnp.zeros_like(rcv_count)

    def pair_step(number):
        ty, j = number // PLANE, lax.rem(number, PLANE)
        values = index_landed[number].astype(jnp.float32)
        shots = jnp.concatenate([one_hot(values[r : r + 1], ids) for r in range(tiles)], axis=1)
        rcvs = jnp.concatenate([one_hot(values[tiles + r : tiles + r + 1], ids) for r in range(tiles)], axis=1)
        pair = lax.dot_general(shots, rcvs, NT, preferred_element_type=jnp.float32)
        across = pl.ds(pl.multiple_of(j * LANES, LANES), LANES)
        pairs[pl.ds(pl.multiple_of(ty * LANES, LANES), LANES), across] = pair.astype(jnp.bfloat16)
        totals[ty] += pair
        rcv_count[:, across] += jnp.broadcast_to(pair.sum(axis=0, keepdims=True), (8, LANES))

    pair_step(me)

    def pair_loop(k, carry):
        index_copy(k, None).wait()
        pair_step(other(k, place)[2])
        return carry

    lax.fori_loop(1, CHIPS, pair_loop, 0)

    def pair_copy(src, dst, n):
        return pltpu.make_async_remote_copy(
            src, dst, part_sems.at[0, n], part_sems.at[1, n], device_id=partner, device_id_type=MESH
        )

    count_copy = pair_copy(rcv_count, count_land, SWEEPS)
    count_copy.start()
    counts = jnp.concatenate([totals[b].T.sum(axis=0, keepdims=True) for b in range(RINGS)], axis=1)

    def block_wait(k, carry):
        number = other(k, place)[2]
        block_copy(number, number).wait()
        return carry

    lax.fori_loop(1, CHIPS, block_wait, 0)
    shot_logs = jnp.concatenate(
        [landed[b * PLANE : (b + 1) * PLANE, :OWNED, :].sum(axis=0) for b in range(RINGS)], axis=1
    )
    rcv_logs = landed[:PLANE, OWNED:, :]
    for b in range(1, RINGS):
        rcv_logs = rcv_logs + landed[b * PLANE : (b + 1) * PLANE, OWNED:, :]
    rcv_logs = jnp.concatenate([rcv_logs[j] for j in range(PLANE)], axis=1)
    count_copy.wait()
    rcv_counts = rcv_count[0:1, :] + count_land[0:1, :]
    copies = [pair_copy(part_send.at[n], part_land.at[n], n) for n in range(SWEEPS)]

    def copy_to(src, dst, kind, k, sending):
        ty, rcv, number, device = other(k, place)
        at = me if sending else number
        source = src.at[ty] if kind == 0 else src.at[rcv]
        return pltpu.make_async_remote_copy(
            source, dst.at[at], term_sems.at[2 * kind, number], term_sems.at[2 * kind + 1, at],
            device_id=device, device_id_type=MESH
        )

    def send_all(src, dst, kind):
        def step(k, carry):
            copy_to(src, dst, kind, k, True).start()
            return carry

        lax.fori_loop(1, CHIPS, step, 0)

    rcv_terms = None
    for n in range(SWEEPS):
        if n == 0:
            shot_terms = shot_logs / counts
        else:
            both = lax.dot_general(two_parts(rcv_terms, 0), pairs[...], NT, preferred_element_type=jnp.float32)
            shot_terms = (shot_logs - (both[:OWNED] + both[OWNED:])) / counts
        if n == SWEEPS - 1:
            for b in range(RINGS):
                shot_send[b] = shot_terms[:, b * LANES : (b + 1) * LANES]
            send_all(shot_send, shot_land, 0)
        both = jnp.dot(two_parts(shot_terms, 0), pairs[...], preferred_element_type=jnp.float32)
        part = rcv_logs - (both[:OWNED] + both[OWNED:])
        part_send[n] = part
        copies[n].start()
        copies[n].wait()
        rcv_terms = (part + part_land[n]) / rcv_counts
    for j in range(PLANE):
        rcv_send[j] = rcv_terms[:, j * LANES : (j + 1) * LANES]
    send_all(rcv_send, rcv_land, 1)
    shot_land[me] = shot_send[y]
    rcv_land[me] = rcv_send[mine]

    def finish(k, carry):
        copy_to(shot_send, shot_land, 0, k, False).wait()
        copy_to(rcv_send, rcv_land, 1, k, False).wait()
        return carry

    lax.fori_loop(1, CHIPS, finish, 0)
    shot_out[...] = shot_land[...]
    rcv_out[...] = rcv_land[...]


def turn_kernel(shot_in, rcv_in, shot_out, rcv_out, order):
    half = order.shape[0] // 2
    for src, dst in ((shot_in, shot_out), (rcv_in, rcv_out)):
        order[pl.ds(0, half, stride=2), :] = src[:half]
        order[pl.ds(1, half, stride=2), :] = src[half:]
        dst[...] = order[...].T


def shards(traces, trace_shot, trace_rcv, fold_count):
    slots, samples = traces.shape[2:]
    bins = samples // 2
    tiles = slots // LANES
    rows_np, turns_np = phase_tables(samples)
    alive = jnp.arange(slots, dtype=jnp.int32).reshape(1, tiles, LANES) < fold_count[0, 0]
    index = jnp.stack([trace_shot[0, 0], trace_rcv[0, 0]]).reshape(2, tiles, LANES)
    index = jnp.where(alive, index, -1).reshape(2 * tiles, LANES)
    f32, bf16 = jnp.float32, jnp.bfloat16
    vmem = pl.BlockSpec(memory_space=VMEM)
    shape = jax.ShapeDtypeStruct
    shot_got, rcv_got = pl.pallas_call(
        main_kernel,
        out_shape=(shape((CHIPS, OWNED, LANES), f32), shape((CHIPS, OWNED, LANES), f32)),
        in_specs=[pl.BlockSpec(memory_space=pl.ANY), vmem, vmem, vmem],
        out_specs=(vmem,) * 2,
        scratch_shapes=[
            VMEM((slots, samples), bf16),
            VMEM((samples, 2 * LANES), bf16),
            VMEM((2 * LANES, slots), bf16),
            VMEM((CHIPS, 2 * OWNED, LANES), f32),
            VMEM((CHIPS, 2 * OWNED, LANES), f32),
            VMEM((CHIPS, 2 * tiles, LANES), jnp.int32),
            VMEM((RINGS * LANES, PLANE * LANES), bf16),
            VMEM((RINGS, LANES, LANES), f32),
            VMEM((8, PLANE * LANES), f32),
            VMEM((8, PLANE * LANES), f32),
            VMEM((RINGS, OWNED, LANES), f32),
            VMEM((PLANE, OWNED, LANES), f32),
            VMEM((CHIPS, OWNED, LANES), f32),
            VMEM((CHIPS, OWNED, LANES), f32),
            VMEM((SWEEPS, OWNED, PLANE * LANES), f32),
            VMEM((SWEEPS, OWNED, PLANE * LANES), f32),
            pltpu.SemaphoreType.DMA((slots // 512,)),
            pltpu.SemaphoreType.DMA((4, CHIPS)),
            pltpu.SemaphoreType.DMA((4, CHIPS)),
            pltpu.SemaphoreType.DMA((2, SWEEPS + 1)),
        ],
        compiler_params=pltpu.CompilerParams(
            collective_id=0, has_side_effects=True, vmem_limit_bytes=VMEM_LIMIT
        ),
        name="decompose",
    )(traces[0, 0], index, jnp.asarray(rows_np), jnp.asarray(turns_np))
    return pl.pallas_call(
        turn_kernel,
        out_shape=(shape((LANES, bins), f32), shape((LANES, bins), f32)),
        in_specs=[vmem] * 2,
        out_specs=(vmem,) * 2,
        scratch_shapes=[VMEM((bins, LANES), f32)],
        compiler_params=pltpu.CompilerParams(vmem_limit_bytes=VMEM_LIMIT),
        name="turn",
    )(shot_got.reshape(bins, LANES), rcv_got.reshape(bins, LANES))


def solution(mesh):
    return jax.shard_map(
        shards,
        mesh=mesh,
        in_specs=(
            P("shot", "rcv", None, None),
            P("shot", "rcv", None),
            P("shot", "rcv", None),
            P("shot", "rcv"),
        ),
        out_specs=(P("shot", None), P("rcv", None)),
        check_vma=False,
    )
```

```python
import functools
import math

import jax
import jax.numpy as jnp
import numpy as np
from jax import lax
from jax.experimental import pallas as pl
from jax.experimental.pallas import tpu as pltpu
from jax.sharding import PartitionSpec as P

MESH = pl.DeviceIdType.MESH
VMEM = pltpu.VMEM
SWEEPS = 3
LANES = 128
CHIPS = 64
PLANE = 16
RINGS = 4
OWNED = 16
NT = (((1,), (1,)), ((), ()))
VMEM_LIMIT = 60 * 1024 * 1024


def phase_tables(samples):
    lane = np.arange(LANES)
    wave = lambda steps: np.stack([g(2 * np.pi * (steps % samples) / samples) for g in (np.cos, np.sin)])
    rows = wave(16 * lane[:, None] * lane[None, :])
    sub = np.arange(8)[:, None]
    turns = [[wave((2 * sub + odd) * (LANES * q + lane[None, :])) for odd in range(2)] for q in range(4)]
    return rows.astype(np.float32), np.array(turns).astype(np.float32)


def fill_tables(table, rows_ref, turns_ref, q):
    turns = [[turns_ref[q, odd, part] for part in range(2)] for odd in range(2)]

    def step(m, carry):
        tops = [[], []]
        for part in range(2):
            at = 2 * m + part
            rc = jnp.broadcast_to(rows_ref[0, pl.ds(at, 1), :], (8, LANES))
            rs = jnp.broadcast_to(rows_ref[1, pl.ds(at, 1), :], (8, LANES))
            for odd in range(2):
                turn_c, turn_s = turns[odd]
                tops[odd].append(jnp.concatenate([rc * turn_c - rs * turn_s, rs * turn_c + rc * turn_s], axis=1))
        at = pl.ds(pl.multiple_of(m * 16, 16), 16)
        for odd in range(2):
            table[odd, at, :] = jnp.concatenate(tops[odd], axis=0).astype(jnp.bfloat16)
        return carry

    lax.fori_loop(0, 64, step, 0, unroll=8)

    @pl.when(q == 0)
    def _():
        first = lax.broadcasted_iota(jnp.int32, (8, LANES), 1) == 0
        flip = 1.0 - 2.0 * lax.rem(lax.broadcasted_iota(jnp.int32, (8, LANES), 0), 2).astype(jnp.float32)
        flip = jnp.concatenate([flip, flip], axis=0)
        first = jnp.concatenate([first, first], axis=0)
        for odd in range(2):
            for m in range(64):
                at = pl.ds(m * 16, 16)
                old = table[odd, at, LANES:].astype(jnp.float32)
                table[odd, at, LANES:] = jnp.where(first, flip, old).astype(jnp.bfloat16)


def one_hot(row, ids):
    wide = jnp.broadcast_to(row, (16, LANES)).astype(jnp.bfloat16)
    wide = jnp.concatenate([wide] * 8, axis=0)
    return jnp.where(wide == ids, jnp.ones_like(ids), jnp.zeros_like(ids))


def sublane_ids():
    return lax.broadcasted_iota(jnp.int32, (LANES, LANES), 0).astype(jnp.float32).astype(jnp.bfloat16)


def my_place():
    shot, rcv = lax.axis_index("shot"), lax.axis_index("rcv")
    return shot // 2, lax.rem(shot, 2), rcv // 4, lax.rem(rcv, 4)


def other(k, place):
    y, core, z, x = place
    ty = lax.rem(y + k // 16, 4)
    tz = lax.rem(z + lax.rem(k // 4, 4), 4)
    tx = lax.rem(x + lax.rem(k, 4), 4)
    rcv = tz * 4 + tx
    return ty, rcv, ty * PLANE + rcv, (ty * 2 + core, rcv)


def device_of(number, core):
    return (number // PLANE) * 2 + core, lax.rem(number, PLANE)


def greet(place, partner):
    barrier = pltpu.get_barrier_semaphore()

    def step(k, carry):
        pl.semaphore_signal(barrier, inc=1, device_id=other(k, place)[3], device_id_type=MESH)
        return carry

    lax.fori_loop(1, CHIPS, step, 0)
    pl.semaphore_signal(barrier, inc=1, device_id=partner, device_id_type=MESH)
    return lambda: pl.semaphore_wait(barrier, CHIPS)


def two_parts(value, axis):
    top = value.astype(jnp.bfloat16)
    return jnp.concatenate([top, (value - top.astype(jnp.float32)).astype(jnp.bfloat16)], axis=axis)


def main_kernel(fold, trace_shot, trace_rcv, traces, rows_ref, turns_ref, shot_out, rcv_out,
                index, held, halves, table, hot, blocks, landed, index_landed,
                pairs, totals, rcv_count, count_land,
                shot_send, rcv_send, shot_land, rcv_land, part_send, part_land,
                trace_sem, sems, term_sems, part_sems):
    place = my_place()
    y, core, z, x = place
    mine = z * 4 + x
    me = y * PLANE + mine
    partner = (y * 2 + 1 - core, mine)
    slots, samples = held.shape
    tiles = slots // LANES

    all_here = greet(place, partner)
    block = 512
    loads = [
        pltpu.make_async_copy(traces.at[pl.ds(b * block, block)], held.at[pl.ds(b * block, block)], trace_sem.at[b])
        for b in range(slots // block)
    ]
    for load in loads:
        load.start()
    lane = lax.broadcasted_iota(jnp.int32, (1, LANES), 1)
    for r in range(tiles):
        live = lane + r * LANES < fold[0, 0]
        at = slice(r * LANES, (r + 1) * LANES)
        index[r : r + 1, :] = jnp.where(live, trace_shot[:, at], -1)
        index[tiles + r : tiles + r + 1, :] = jnp.where(live, trace_rcv[:, at], -1)
    ids = sublane_ids()
    values = index[...].astype(jnp.float32)
    for r in range(tiles):
        hot[:LANES, r * LANES : (r + 1) * LANES] = one_hot(values[r : r + 1], ids)
        hot[LANES:, r * LANES : (r + 1) * LANES] = one_hot(values[tiles + r : tiles + r + 1], ids)
    index_landed[me] = index[...]
    wide = 2 * LANES
    rank = lax.broadcasted_iota(jnp.int32, (wide, wide), 0)
    spot = lax.broadcasted_iota(jnp.int32, (wide, wide), 1)
    wanted = jnp.where(spot < LANES, 2 * spot, 2 * (spot - LANES) + 1)
    split = jnp.where(rank == wanted, 1.0, 0.0).astype(jnp.bfloat16)
    for b, load in enumerate(loads):
        load.wait()
        for n in range(samples // wide):
            at = slice(b * block, (b + 1) * block)
            apart = jnp.dot(held[at, n * wide : (n + 1) * wide], split, preferred_element_type=jnp.float32)
            apart = apart.astype(jnp.bfloat16)
            halves[0, at, n * LANES : (n + 1) * LANES] = apart[:, :LANES]
            halves[1, at, n * LANES : (n + 1) * LANES] = apart[:, LANES:]

    def index_copy(k, slot):
        number, device = other(k, place)[2:]
        return pltpu.make_async_remote_copy(
            index, index_landed.at[number if slot is None else slot], sems.at[0, number],
            sems.at[1, number if slot is None else slot], device_id=device, device_id_type=MESH
        )

    def block_copy(number, slot):
        return pltpu.make_async_remote_copy(
            blocks.at[number], landed.at[slot], sems.at[2, number], sems.at[3, slot],
            device_id=device_of(number, core), device_id_type=MESH
        )

    def send_index(k, carry):
        index_copy(k, me).start()
        return carry

    def chunk_step(t, carry):
        q = lax.rem(t + me, 4)
        fill_tables(table, rows_ref, turns_ref, q)
        first = (lax.broadcasted_iota(jnp.int32, (1, LANES), 1) + q) == 0
        sums = [None, None]
        for b in range(slots // block):
            at = slice(b * block, (b + 1) * block)
            even = jnp.dot(halves[0, at], table[0], preferred_element_type=jnp.float32)
            odd = jnp.dot(halves[1, at], table[1], preferred_element_type=jnp.float32)
            even_c, even_s, odd_c, odd_s = even[:, :LANES], even[:, LANES:], odd[:, :LANES], odd[:, LANES:]
            whole = (even_c + odd_c, jnp.where(first, 0.0, even_s + odd_s))
            mirror = (jnp.where(first, even_s, even_c - odd_c), jnp.where(first, odd_s, even_s - odd_s))
            for n, (real, imag) in enumerate((whole, mirror)):
                logs = jnp.log((real * real + imag * imag) * (1.0 / samples) + 1e-6)
                part = jnp.dot(hot[:, at], two_parts(logs, 1), preferred_element_type=jnp.float32)
                sums[n] = part if b == 0 else sums[n] + part
        for n in range(2):
            total = (sums[n][:, :LANES] + sums[n][:, LANES:]).T
            at = pl.ds(q * 16 + n * 8, 8)
            blocks[at, :OWNED, :] = total[:, :LANES].reshape(8, OWNED, LANES)
            blocks[at, OWNED:, :] = total[:, LANES:].reshape(8, OWNED, LANES)

        @pl.when(t == 0)
        def _():
            all_here()
            lax.fori_loop(1, CHIPS, send_index, 0)

        def send(n, inner):
            number = q * 16 + n

            @pl.when(number != me)
            def _():
                block_copy(number, me).start()

            return inner

        lax.fori_loop(0, 16, send, 0)
        return carry

    lax.fori_loop(0, 4, chunk_step, 0)
    landed[me] = blocks[me]

    totals[...] = jnp.zeros_like(totals)

    def index_wait(k, carry):
        index_copy(k, None).wait()
        return carry

    lax.fori_loop(1, CHIPS, index_wait, 0)

    def pair_step(j, carry):
        across = pl.ds(pl.multiple_of(j * LANES, LANES), LANES)
        count = None
        for b in range(RINGS):
            values = index_landed[b * PLANE + j].astype(jnp.float32)
            shots = jnp.concatenate([one_hot(values[r : r + 1], ids) for r in range(tiles)], axis=1)
            rcvs = jnp.concatenate([one_hot(values[tiles + r : tiles + r + 1], ids) for r in range(tiles)], axis=1)
            pair = lax.dot_general(shots, rcvs, NT, preferred_element_type=jnp.float32)
            pairs[b * LANES : (b + 1) * LANES, across] = pair.astype(jnp.bfloat16)
            totals[b] += pair
            count = pair if count is None else count + pair
        rcv_count[:, across] = jnp.broadcast_to(count.sum(axis=0, keepdims=True), (8, LANES))
        return carry

    lax.fori_loop(0, PLANE, pair_step, 0, unroll=2)

    def pair_copy(src, dst, n):
        return pltpu.make_async_remote_copy(
            src, dst, part_sems.at[0, n], part_sems.at[1, n], device_id=partner, device_id_type=MESH
        )

    count_copy = pair_copy(rcv_count, count_land, SWEEPS)
    count_copy.start()
    counts = jnp.concatenate([totals[b].T.sum(axis=0, keepdims=True) for b in range(RINGS)], axis=1)

    def block_wait(k, carry):
        number = other(k, place)[2]
        block_copy(number, number).wait()
        return carry

    lax.fori_loop(1, CHIPS, block_wait, 0)
    shot_logs = jnp.concatenate(
        [landed[b * PLANE : (b + 1) * PLANE, :OWNED, :].sum(axis=0) for b in range(RINGS)], axis=1
    )
    rcv_logs = landed[:PLANE, OWNED:, :]
    for b in range(1, RINGS):
        rcv_logs = rcv_logs + landed[b * PLANE : (b + 1) * PLANE, OWNED:, :]
    rcv_logs = jnp.concatenate([rcv_logs[j] for j in range(PLANE)], axis=1)
    count_copy.wait()
    rcv_counts = rcv_count[0:1, :] + count_land[0:1, :]
    copies = [pair_copy(part_send.at[n], part_land.at[n], n) for n in range(SWEEPS)]

    def copy_to(src, dst, kind, k, sending):
        ty, rcv, number, device = other(k, place)
        at = me if sending else number
        source = src.at[ty] if kind == 0 else src.at[rcv]
        return pltpu.make_async_remote_copy(
            source, dst.at[at], term_sems.at[2 * kind, number], term_sems.at[2 * kind + 1, at],
            device_id=device, device_id_type=MESH
        )

    def send_all(src, dst, kind):
        def step(k, carry):
            copy_to(src, dst, kind, k, True).start()
            return carry

        lax.fori_loop(1, CHIPS, step, 0)

    rcv_terms = None
    for n in range(SWEEPS):
        if n == 0:
            shot_terms = shot_logs / counts
        else:
            both = lax.dot_general(two_parts(rcv_terms, 0), pairs[...], NT, preferred_element_type=jnp.float32)
            shot_terms = (shot_logs - (both[:OWNED] + both[OWNED:])) / counts
        if n == SWEEPS - 1:
            for b in range(RINGS):
                shot_send[b] = shot_terms[:, b * LANES : (b + 1) * LANES]
            send_all(shot_send, shot_land, 0)
        both = jnp.dot(two_parts(shot_terms, 0), pairs[...], preferred_element_type=jnp.float32)
        part = rcv_logs - (both[:OWNED] + both[OWNED:])
        part_send[n] = part
        copies[n].start()
        copies[n].wait()
        rcv_terms = (part + part_land[n]) / rcv_counts
    for j in range(PLANE):
        rcv_send[j] = rcv_terms[:, j * LANES : (j + 1) * LANES]
    send_all(rcv_send, rcv_land, 1)
    shot_land[me] = shot_send[y]
    rcv_land[me] = rcv_send[mine]

    def finish(k, carry):
        copy_to(shot_send, shot_land, 0, k, False).wait()
        copy_to(rcv_send, rcv_land, 1, k, False).wait()
        return carry

    lax.fori_loop(1, CHIPS, finish, 0)
    shot_out[...] = shot_land[...]
    rcv_out[...] = rcv_land[...]


def turn_kernel(shot_in, rcv_in, shot_out, rcv_out):
    lane = lax.broadcasted_iota(jnp.int32, (LANES, LANES), 1)
    back = lax.rem(LANES - lane, LANES)
    for src, dst in ((shot_in, shot_out), (rcv_in, rcv_out)):
        mirrors = []
        for q in range(4):
            at = 2 * q * LANES
            dst[:, q * LANES : (q + 1) * LANES] = src[at : at + LANES].T
            mirrors.append(jnp.take_along_axis(src[at + LANES : at + 2 * LANES].T, back, axis=1))
        for c in range(4, 8):
            head = mirrors[8 - c if c > 4 else 0]
            dst[:, c * LANES : (c + 1) * LANES] = jnp.where(lane == 0, head, mirrors[7 - c])


def shards(traces, trace_shot, trace_rcv, fold_count):
    slots, samples = traces.shape[2:]
    bins = samples // 2
    tiles = slots // LANES
    rows_np, turns_np = phase_tables(samples)
    f32, bf16 = jnp.float32, jnp.bfloat16
    vmem = pl.BlockSpec(memory_space=VMEM)
    shape = jax.ShapeDtypeStruct
    shot_got, rcv_got = pl.pallas_call(
        main_kernel,
        out_shape=(shape((CHIPS, OWNED, LANES), f32), shape((CHIPS, OWNED, LANES), f32)),
        in_specs=[pl.BlockSpec(memory_space=pltpu.SMEM), vmem, vmem, pl.BlockSpec(memory_space=pl.ANY), vmem, vmem],
        out_specs=(vmem,) * 2,
        scratch_shapes=[
            VMEM((2 * tiles, LANES), jnp.int32),
            VMEM((slots, samples), bf16),
            VMEM((2, slots, samples // 2), bf16),
            VMEM((2, samples // 2, 2 * LANES), bf16),
            VMEM((2 * LANES, slots), bf16),
            VMEM((CHIPS, 2 * OWNED, LANES), f32),
            VMEM((CHIPS, 2 * OWNED, LANES), f32),
            VMEM((CHIPS, 2 * tiles, LANES), jnp.int32),
            VMEM((RINGS * LANES, PLANE * LANES), bf16),
            VMEM((RINGS, LANES, LANES), f32),
            VMEM((8, PLANE * LANES), f32),
            VMEM((8, PLANE * LANES), f32),
            VMEM((RINGS, OWNED, LANES), f32),
            VMEM((PLANE, OWNED, LANES), f32),
            VMEM((CHIPS, OWNED, LANES), f32),
            VMEM((CHIPS, OWNED, LANES), f32),
            VMEM((SWEEPS, OWNED, PLANE * LANES), f32),
            VMEM((SWEEPS, OWNED, PLANE * LANES), f32),
            pltpu.SemaphoreType.DMA((slots // 512,)),
            pltpu.SemaphoreType.DMA((4, CHIPS)),
            pltpu.SemaphoreType.DMA((4, CHIPS)),
            pltpu.SemaphoreType.DMA((2, SWEEPS + 1)),
        ],
        compiler_params=pltpu.CompilerParams(
            collective_id=0, has_side_effects=True, vmem_limit_bytes=VMEM_LIMIT
        ),
        name="decompose",
    )(fold_count, trace_shot[0], trace_rcv[0], traces[0, 0], jnp.asarray(rows_np), jnp.asarray(turns_np))
    return pl.pallas_call(
        turn_kernel,
        out_shape=(shape((LANES, bins), f32), shape((LANES, bins), f32)),
        in_specs=[vmem] * 2,
        out_specs=(vmem,) * 2,
        compiler_params=pltpu.CompilerParams(vmem_limit_bytes=VMEM_LIMIT),
        name="turn",
    )(shot_got.reshape(bins, LANES), rcv_got.reshape(bins, LANES))


def solution(mesh):
    return jax.shard_map(
        shards,
        mesh=mesh,
        in_specs=(
            P("shot", "rcv", None, None),
            P("shot", "rcv", None),
            P("shot", "rcv", None),
            P("shot", "rcv"),
        ),
        out_specs=(P("shot", None), P("rcv", None)),
        check_vma=False,
    )
```

```python
import functools
import math

import jax
import jax.numpy as jnp
import numpy as np
from jax import lax
from jax.experimental import pallas as pl
from jax.experimental.pallas import tpu as pltpu
from jax.sharding import PartitionSpec as P

MESH = pl.DeviceIdType.MESH
VMEM = pltpu.VMEM
SWEEPS = 3
LANES = 128
CHIPS = 64
PLANE = 16
RINGS = 4
OWNED = 16
NT = (((1,), (1,)), ((), ()))
VMEM_LIMIT = 60 * 1024 * 1024


def phase_tables(samples):
    lane = np.arange(LANES)
    wave = lambda steps: np.stack([g(2 * np.pi * (steps % samples) / samples) for g in (np.cos, np.sin)])
    rows = wave(16 * lane[:, None] * lane[None, :])
    sub = np.arange(8)[:, None]
    turns = [[wave((2 * sub + odd) * (LANES * q + lane[None, :])) for odd in range(2)] for q in range(4)]
    return rows.astype(np.float32), np.array(turns).astype(np.float32)


def fill_tables(table, rows_ref, turns_ref, q):
    turns = [[turns_ref[q, odd, part] for part in range(2)] for odd in range(2)]

    def step(m, carry):
        tops = [[], []]
        for part in range(2):
            at = 2 * m + part
            rc = jnp.broadcast_to(rows_ref[0, pl.ds(at, 1), :], (8, LANES))
            rs = jnp.broadcast_to(rows_ref[1, pl.ds(at, 1), :], (8, LANES))
            for odd in range(2):
                turn_c, turn_s = turns[odd]
                tops[odd].append(jnp.concatenate([rc * turn_c - rs * turn_s, rs * turn_c + rc * turn_s], axis=1))
        at = pl.ds(pl.multiple_of(m * 16, 16), 16)
        for odd in range(2):
            table[odd, at, :] = jnp.concatenate(tops[odd], axis=0).astype(jnp.bfloat16)
        return carry

    lax.fori_loop(0, 64, step, 0, unroll=8)

    @pl.when(q == 0)
    def _():
        first = lax.broadcasted_iota(jnp.int32, (8, LANES), 1) == 0
        flip = 1.0 - 2.0 * lax.rem(lax.broadcasted_iota(jnp.int32, (8, LANES), 0), 2).astype(jnp.float32)
        flip = jnp.concatenate([flip, flip], axis=0)
        first = jnp.concatenate([first, first], axis=0)
        for odd in range(2):
            for m in range(64):
                at = pl.ds(m * 16, 16)
                old = table[odd, at, LANES:].astype(jnp.float32)
                table[odd, at, LANES:] = jnp.where(first, flip, old).astype(jnp.bfloat16)


def one_hot(row, ids):
    wide = jnp.broadcast_to(row, (16, LANES)).astype(jnp.bfloat16)
    wide = jnp.concatenate([wide] * 8, axis=0)
    return jnp.where(wide == ids, jnp.ones_like(ids), jnp.zeros_like(ids))


def sublane_ids():
    return lax.broadcasted_iota(jnp.int32, (LANES, LANES), 0).astype(jnp.float32).astype(jnp.bfloat16)


def my_place():
    shot, rcv = lax.axis_index("shot"), lax.axis_index("rcv")
    return shot // 2, lax.rem(shot, 2), rcv // 4, lax.rem(rcv, 4)


def others(place):
    y, core, z, x = place
    ys, zs, xs = ([lax.rem(at + d, RINGS) for d in range(RINGS)] for at in (y, z, x))
    found = []
    for k in range(1, CHIPS):
        ty, rcv = ys[k // PLANE], zs[k // 4 % 4] * 4 + xs[k % 4]
        found.append((ty, rcv, ty * PLANE + rcv, (ty * 2 + core, rcv)))
    return found


def two_parts(value, axis):
    top = value.astype(jnp.bfloat16)
    return jnp.concatenate([top, (value - top.astype(jnp.float32)).astype(jnp.bfloat16)], axis=axis)


def main_kernel(fold, trace_shot, trace_rcv, traces, rows_ref, turns_ref, shot_out, rcv_out,
                index, held, halves, table, hot, shot_blocks, rcv_blocks, pre_send, pre_land,
                shot_landed, rcv_landed, index_landed,
                pairs, totals, rcv_count, count_land,
                shot_send, rcv_send, shot_land, rcv_land, part_send, part_land,
                trace_sem, sems, pre_sems, part_sems):
    place = my_place()
    y, core, z, x = place
    mine = z * 4 + x
    me = y * PLANE + mine
    partner = (y * 2 + 1 - core, mine)
    slots, samples = held.shape
    tiles = slots // LANES
    away = others(place)

    barrier = pltpu.get_barrier_semaphore()
    for device in [a[3] for a in away] + [partner]:
        pl.semaphore_signal(barrier, inc=1, device_id=device, device_id_type=MESH)

    def send(src, dst, kind, device):
        pltpu.make_async_remote_copy(
            src, dst, sems.at[0, kind], sems.at[1, kind], device_id=device, device_id_type=MESH
        ).start()

    def settle(ref, kind, way):
        span = ref.at[pl.ds(0, CHIPS - 1)]
        pltpu.make_async_copy(span, span, sems.at[way, kind]).wait()

    block = 512
    loads = [
        pltpu.make_async_copy(traces.at[pl.ds(b * block, block)], held.at[pl.ds(b * block, block)], trace_sem.at[b])
        for b in range(slots // block)
    ]
    for load in loads:
        load.start()
    lane = lax.broadcasted_iota(jnp.int32, (1, LANES), 1)
    for r in range(tiles):
        live = lane + r * LANES < fold[0, 0]
        at = slice(r * LANES, (r + 1) * LANES)
        index[r : r + 1, :] = jnp.where(live, trace_shot[:, at], -1)
        index[tiles + r : tiles + r + 1, :] = jnp.where(live, trace_rcv[:, at], -1)
    ids = sublane_ids()
    values = index[...].astype(jnp.float32)
    for r in range(tiles):
        hot[:LANES, r * LANES : (r + 1) * LANES] = one_hot(values[r : r + 1], ids)
        hot[LANES:, r * LANES : (r + 1) * LANES] = one_hot(values[tiles + r : tiles + r + 1], ids)
    index_landed[me] = index[...]
    wide = 2 * LANES
    rank = lax.broadcasted_iota(jnp.int32, (wide, wide), 0)
    spot = lax.broadcasted_iota(jnp.int32, (wide, wide), 1)
    wanted = jnp.where(spot < LANES, 2 * spot, 2 * (spot - LANES) + 1)
    split = jnp.where(rank == wanted, 1.0, 0.0).astype(jnp.bfloat16)
    for b, load in enumerate(loads):
        load.wait()
        for n in range(samples // wide):
            at = slice(b * block, (b + 1) * block)
            apart = jnp.dot(held[at, n * wide : (n + 1) * wide], split, preferred_element_type=jnp.float32)
            apart = apart.astype(jnp.bfloat16)
            halves[0, at, n * LANES : (n + 1) * LANES] = apart[:, :LANES]
            halves[1, at, n * LANES : (n + 1) * LANES] = apart[:, LANES:]

    def pre_copy(t):
        return pltpu.make_async_remote_copy(
            pre_send.at[t], pre_land.at[t], pre_sems.at[0, t], pre_sems.at[1, t],
            device_id=partner, device_id_type=MESH
        )

    def send_rcv(t):
        q = lax.rem(t + me, RINGS)
        pre_copy(t).wait()
        at = pl.ds(q * PLANE, PLANE)
        rcv_blocks[at] = rcv_blocks[at] + pre_land[t]
        for n in range(PLANE):

            @pl.when(q * PLANE + n != me)
            def _():
                send(rcv_blocks.at[q * PLANE + n], rcv_landed.at[me], 2, (q * 2 + core, n))

    def chunk_step(t, carry):
        q = lax.rem(t + me, 4)
        fill_tables(table, rows_ref, turns_ref, q)
        first = (lax.broadcasted_iota(jnp.int32, (1, LANES), 1) + q) == 0
        sums = [None, None]
        for b in range(slots // block):
            at = slice(b * block, (b + 1) * block)
            even = jnp.dot(halves[0, at], table[0], preferred_element_type=jnp.float32)
            odd = jnp.dot(halves[1, at], table[1], preferred_element_type=jnp.float32)
            even_c, even_s, odd_c, odd_s = even[:, :LANES], even[:, LANES:], odd[:, :LANES], odd[:, LANES:]
            whole = (even_c + odd_c, jnp.where(first, 0.0, even_s + odd_s))
            mirror = (jnp.where(first, even_s, even_c - odd_c), jnp.where(first, odd_s, even_s - odd_s))
            for n, (real, imag) in enumerate((whole, mirror)):
                logs = jnp.log((real * real + imag * imag) * (1.0 / samples) + 1e-6)
                part = jnp.dot(hot[:, at], two_parts(logs, 1), preferred_element_type=jnp.float32)
                sums[n] = part if b == 0 else sums[n] + part
        for n in range(2):
            total = (sums[n][:, :LANES] + sums[n][:, LANES:]).T
            shot_blocks[pl.ds(q * PLANE + n * 8, 8)] = total[:, :LANES].reshape(8, OWNED, LANES)
            both = total[:, LANES:].reshape(8, 2, OWNED // 2, LANES)
            rcv_blocks[pl.ds(q * PLANE + n * 8, 8)] = jnp.where(core == 0, both[:, 0], both[:, 1])
            pre_send[t, n * 8 : n * 8 + 8] = jnp.where(core == 0, both[:, 1], both[:, 0])

        @pl.when(t == 0)
        def _():
            pl.semaphore_wait(barrier, CHIPS)
            for _, _, _, device in away:
                send(index, index_landed.at[me], 0, device)

        pre_copy(t).start()
        for n in range(PLANE):

            @pl.when(q * PLANE + n != me)
            def _():
                send(shot_blocks.at[q * PLANE + n], shot_landed.at[me], 1, (q * 2 + core, n))

        @pl.when(t > 0)
        def _():
            send_rcv(t - 1)

        return carry

    lax.fori_loop(0, RINGS, chunk_step, 0)
    shot_landed[me] = shot_blocks[me]

    totals[...] = jnp.zeros_like(totals)

    settle(index_landed, 0, 1)

    def pair_step(j, carry):
        across = pl.ds(pl.multiple_of(j * LANES, LANES), LANES)
        count = None
        for b in range(RINGS):
            values = index_landed[b * PLANE + j].astype(jnp.float32)
            shots = jnp.concatenate([one_hot(values[r : r + 1], ids) for r in range(tiles)], axis=1)
            rcvs = jnp.concatenate([one_hot(values[tiles + r : tiles + r + 1], ids) for r in range(tiles)], axis=1)
            pair = lax.dot_general(shots, rcvs, NT, preferred_element_type=jnp.float32)
            pairs[b * LANES : (b + 1) * LANES, across] = pair.astype(jnp.bfloat16)
            totals[b] += pair
            count = pair if count is None else count + pair
        rcv_count[:, across] = jnp.broadcast_to(count.sum(axis=0, keepdims=True), (8, LANES))
        return carry

    lax.fori_loop(0, 4, pair_step, 0, unroll=2)
    send_rcv(RINGS - 1)
    rcv_landed[me] = rcv_blocks[me]
    lax.fori_loop(4, PLANE, pair_step, 0, unroll=2)

    def pair_copy(src, dst, n):
        return pltpu.make_async_remote_copy(
            src, dst, part_sems.at[0, n], part_sems.at[1, n], device_id=partner, device_id_type=MESH
        )

    count_copy = pair_copy(rcv_count, count_land, SWEEPS)
    count_copy.start()
    counts = jnp.concatenate([totals[b].T.sum(axis=0, keepdims=True) for b in range(RINGS)], axis=1)

    settle(shot_landed, 1, 1)
    settle(rcv_landed, 2, 1)
    shot_logs = jnp.concatenate(
        [shot_landed[b * PLANE : (b + 1) * PLANE].sum(axis=0) for b in range(RINGS)], axis=1
    )
    rcv_logs = rcv_landed[:PLANE]
    for b in range(1, RINGS):
        rcv_logs = rcv_logs + rcv_landed[b * PLANE : (b + 1) * PLANE]
    rcv_logs = jnp.concatenate([rcv_logs[j] for j in range(PLANE)], axis=1)
    rcv_logs = jnp.concatenate(
        [jnp.where(core == 0, rcv_logs, 0.0), jnp.where(core == 0, 0.0, rcv_logs)], axis=0
    )
    count_copy.wait()
    rcv_counts = rcv_count[0:1, :] + count_land[0:1, :]
    copies = [pair_copy(part_send.at[n], part_land.at[n], n) for n in range(SWEEPS)]

    rcv_terms = None
    for n in range(SWEEPS):
        if n == 0:
            shot_terms = shot_logs / counts
        else:
            both = lax.dot_general(two_parts(rcv_terms, 0), pairs[...], NT, preferred_element_type=jnp.float32)
            shot_terms = (shot_logs - (both[:OWNED] + both[OWNED:])) / counts
        if n == SWEEPS - 1:
            for b in range(RINGS):
                shot_send[b] = shot_terms[:, b * LANES : (b + 1) * LANES]
            for ty, _, _, device in away:
                send(shot_send.at[ty], shot_land.at[me], 3, device)
        both = jnp.dot(two_parts(shot_terms, 0), pairs[...], preferred_element_type=jnp.float32)
        part = rcv_logs - (both[:OWNED] + both[OWNED:])
        part_send[n] = part
        copies[n].start()
        copies[n].wait()
        rcv_terms = (part + part_land[n]) / rcv_counts
    own = jnp.where(core == 0, rcv_terms[: OWNED // 2], rcv_terms[OWNED // 2 :])
    for j in range(PLANE):
        rcv_send[j] = own[:, j * LANES : (j + 1) * LANES]
    for _, rcv, _, device in away:
        send(rcv_send.at[rcv], rcv_land.at[core, me], 4, device)
    shot_land[me] = shot_send[y]
    rcv_land[core, me] = rcv_send[mine]
    settle(rcv_land.at[core], 4, 1)
    across = pair_copy(rcv_land.at[core], rcv_land.at[core], SWEEPS + 1)
    across.start()
    settle(shot_land, 3, 1)
    shot_out[...] = shot_land[...]
    for kind, ref in enumerate((index_landed, shot_landed, rcv_landed, shot_land, rcv_landed)):
        settle(ref, kind, 0)
    across.wait()
    rcv_out[...] = rcv_land[...]


def turn_kernel(shot_in, rcv_in, shot_out, rcv_out):
    lane = lax.broadcasted_iota(jnp.int32, (LANES, LANES), 1)
    back = lax.rem(LANES - lane, LANES)
    def chunk(src, n):
        if src.shape[0] == CHIPS:
            bins = src[n * 8 : n * 8 + 8]
        else:
            bins = jnp.stack([src[0, n * 8 : n * 8 + 8], src[1, n * 8 : n * 8 + 8]], axis=1)
        return bins.reshape(LANES, LANES).T

    for src, dst in ((shot_in, shot_out), (rcv_in, rcv_out)):
        mirrors = []
        for q in range(4):
            dst[:, q * LANES : (q + 1) * LANES] = chunk(src, 2 * q)
            mirrors.append(jnp.take_along_axis(chunk(src, 2 * q + 1), back, axis=1))
        for c in range(4, 8):
            head = mirrors[8 - c if c > 4 else 0]
            dst[:, c * LANES : (c + 1) * LANES] = jnp.where(lane == 0, head, mirrors[7 - c])


def shards(traces, trace_shot, trace_rcv, fold_count):
    slots, samples = traces.shape[2:]
    bins = samples // 2
    tiles = slots // LANES
    rows_np, turns_np = phase_tables(samples)
    f32, bf16 = jnp.float32, jnp.bfloat16
    vmem = pl.BlockSpec(memory_space=VMEM)
    shape = jax.ShapeDtypeStruct
    shot_got, rcv_got = pl.pallas_call(
        main_kernel,
        out_shape=(shape((CHIPS, OWNED, LANES), f32), shape((2, CHIPS, OWNED // 2, LANES), f32)),
        in_specs=[pl.BlockSpec(memory_space=pltpu.SMEM), vmem, vmem, pl.BlockSpec(memory_space=pl.ANY), vmem, vmem],
        out_specs=(vmem,) * 2,
        scratch_shapes=[
            VMEM((2 * tiles, LANES), jnp.int32),
            VMEM((slots, samples), bf16),
            VMEM((2, slots, samples // 2), bf16),
            VMEM((2, samples // 2, 2 * LANES), bf16),
            VMEM((2 * LANES, slots), bf16),
            VMEM((CHIPS, OWNED, LANES), f32),
            VMEM((CHIPS, OWNED // 2, LANES), f32),
            VMEM((RINGS, PLANE, OWNED // 2, LANES), f32),
            VMEM((RINGS, PLANE, OWNED // 2, LANES), f32),
            VMEM((CHIPS, OWNED, LANES), f32),
            VMEM((CHIPS, OWNED // 2, LANES), f32),
            VMEM((CHIPS, 2 * tiles, LANES), jnp.int32),
            VMEM((RINGS * LANES, PLANE * LANES), bf16),
            VMEM((RINGS, LANES, LANES), f32),
            VMEM((8, PLANE * LANES), f32),
            VMEM((8, PLANE * LANES), f32),
            VMEM((RINGS, OWNED, LANES), f32),
            VMEM((PLANE, OWNED // 2, LANES), f32),
            VMEM((CHIPS, OWNED, LANES), f32),
            VMEM((2, CHIPS, OWNED // 2, LANES), f32),
            VMEM((SWEEPS, OWNED, PLANE * LANES), f32),
            VMEM((SWEEPS, OWNED, PLANE * LANES), f32),
            pltpu.SemaphoreType.DMA((slots // 512,)),
            pltpu.SemaphoreType.DMA((2, 5)),
            pltpu.SemaphoreType.DMA((2, RINGS)),
            pltpu.SemaphoreType.DMA((2, SWEEPS + 2)),
        ],
        compiler_params=pltpu.CompilerParams(
            collective_id=0, has_side_effects=True, vmem_limit_bytes=VMEM_LIMIT
        ),
        name="decompose",
    )(fold_count, trace_shot[0], trace_rcv[0], traces[0, 0], jnp.asarray(rows_np), jnp.asarray(turns_np))
    return pl.pallas_call(
        turn_kernel,
        out_shape=(shape((LANES, bins), f32), shape((LANES, bins), f32)),
        in_specs=[vmem] * 2,
        out_specs=(vmem,) * 2,
        compiler_params=pltpu.CompilerParams(vmem_limit_bytes=VMEM_LIMIT),
        name="turn",
    )(shot_got, rcv_got)


def solution(mesh):
    return jax.shard_map(
        shards,
        mesh=mesh,
        in_specs=(
            P("shot", "rcv", None, None),
            P("shot", "rcv", None),
            P("shot", "rcv", None),
            P("shot", "rcv"),
        ),
        out_specs=(P("shot", None), P("rcv", None)),
        check_vma=False,
    )
```

```python
import functools
import math

import jax
import jax.numpy as jnp
import numpy as np
from jax import lax
from jax.experimental import pallas as pl
from jax.experimental.pallas import tpu as pltpu
from jax.sharding import PartitionSpec as P

MESH = pl.DeviceIdType.MESH
VMEM = pltpu.VMEM
SWEEPS = 3
LANES = 128
CHIPS = 64
PLANE = 16
RINGS = 4
OWNED = 16
NT = (((1,), (1,)), ((), ()))
VMEM_LIMIT = 60 * 1024 * 1024


def phase_tables(samples):
    lane = np.arange(LANES)
    wave = lambda steps: np.stack([g(2 * np.pi * (steps % samples) / samples) for g in (np.cos, np.sin)])
    rows = wave(16 * lane[:, None] * lane[None, :])
    sub = np.arange(8)[:, None]
    turns = [[wave((2 * sub + odd) * (LANES * q + lane[None, :])) for odd in range(2)] for q in range(4)]
    return rows.astype(np.float32), np.array(turns).astype(np.float32)


def fill_tables(table, rows_ref, turns_ref, q):
    turns = [[turns_ref[q, odd, part] for part in range(2)] for odd in range(2)]

    def step(m, carry):
        tops = [[], []]
        for part in range(2):
            at = 2 * m + part
            rc = jnp.broadcast_to(rows_ref[0, pl.ds(at, 1), :], (8, LANES))
            rs = jnp.broadcast_to(rows_ref[1, pl.ds(at, 1), :], (8, LANES))
            for odd in range(2):
                turn_c, turn_s = turns[odd]
                tops[odd].append(jnp.concatenate([rc * turn_c - rs * turn_s, rs * turn_c + rc * turn_s], axis=1))
        at = pl.ds(pl.multiple_of(m * 16, 16), 16)
        for odd in range(2):
            table[odd, at, :] = jnp.concatenate(tops[odd], axis=0).astype(jnp.bfloat16)
        return carry

    lax.fori_loop(0, 64, step, 0, unroll=8)

    @pl.when(q == 0)
    def _():
        first = lax.broadcasted_iota(jnp.int32, (8, LANES), 1) == 0
        flip = 1.0 - 2.0 * lax.rem(lax.broadcasted_iota(jnp.int32, (8, LANES), 0), 2).astype(jnp.float32)
        flip = jnp.concatenate([flip, flip], axis=0)
        first = jnp.concatenate([first, first], axis=0)
        for odd in range(2):
            for m in range(64):
                at = pl.ds(m * 16, 16)
                old = table[odd, at, LANES:].astype(jnp.float32)
                table[odd, at, LANES:] = jnp.where(first, flip, old).astype(jnp.bfloat16)


def one_hot(row, ids):
    wide = jnp.broadcast_to(row, (16, LANES)).astype(jnp.bfloat16)
    wide = jnp.concatenate([wide] * 8, axis=0)
    return jnp.where(wide == ids, jnp.ones_like(ids), jnp.zeros_like(ids))


def sublane_ids():
    return lax.broadcasted_iota(jnp.int32, (LANES, LANES), 0).astype(jnp.float32).astype(jnp.bfloat16)


def my_place():
    shot, rcv = lax.axis_index("shot"), lax.axis_index("rcv")
    return shot // 2, lax.rem(shot, 2), rcv // 4, lax.rem(rcv, 4)


def others(place):
    y, core, z, x = place
    ys, zs, xs = ([lax.rem(at + d, RINGS) for d in range(RINGS)] for at in (y, z, x))
    found = []
    for k in range(1, CHIPS):
        ty, rcv = ys[k // PLANE], zs[k // 4 % 4] * 4 + xs[k % 4]
        found.append((ty, rcv, ty * PLANE + rcv, (ty * 2 + core, rcv)))
    return found


def two_parts(value, axis):
    top = value.astype(jnp.bfloat16)
    return jnp.concatenate([top, (value - top.astype(jnp.float32)).astype(jnp.bfloat16)], axis=axis)


def main_kernel(fold, trace_shot, trace_rcv, traces, rows_ref, turns_ref, shot_out, rcv_out,
                index, held, halves, table, hot, shot_blocks, rcv_blocks, pre_send, pre_land,
                shot_landed, rcv_landed, index_landed,
                pairs, totals, rcv_count, count_land,
                shot_send, rcv_send, shot_land, rcv_land, part_send, part_land,
                trace_sem, index_sems, sems, pre_sems, part_sems):
    place = my_place()
    y, core, z, x = place
    mine = z * 4 + x
    me = y * PLANE + mine
    partner = (y * 2 + 1 - core, mine)
    slots, samples = held.shape
    tiles = slots // LANES
    away = others(place)

    barrier = pltpu.get_barrier_semaphore()
    for device in [a[3] for a in away] + [partner]:
        pl.semaphore_signal(barrier, inc=1, device_id=device, device_id_type=MESH)

    def send(src, dst, kind, device):
        pltpu.make_async_remote_copy(
            src, dst, sems.at[0, kind], sems.at[1, kind], device_id=device, device_id_type=MESH
        ).start()

    def settle(ref, kind, way):
        span = ref.at[pl.ds(0, CHIPS - 1)]
        pltpu.make_async_copy(span, span, sems.at[way, kind]).wait()

    block = 512
    loads = [
        pltpu.make_async_copy(traces.at[pl.ds(b * block, block)], held.at[pl.ds(b * block, block)], trace_sem.at[b])
        for b in range(slots // block)
    ]
    for load in loads:
        load.start()
    lane = lax.broadcasted_iota(jnp.int32, (1, LANES), 1)
    for r in range(tiles):
        live = lane + r * LANES < fold[0, 0]
        at = slice(r * LANES, (r + 1) * LANES)
        index[r : r + 1, :] = jnp.where(live, trace_shot[:, at], -1)
        index[tiles + r : tiles + r + 1, :] = jnp.where(live, trace_rcv[:, at], -1)
    ids = sublane_ids()
    values = index[...].astype(jnp.float32)
    for r in range(tiles):
        hot[:LANES, r * LANES : (r + 1) * LANES] = one_hot(values[r : r + 1], ids)
        hot[LANES:, r * LANES : (r + 1) * LANES] = one_hot(values[tiles + r : tiles + r + 1], ids)
    for part in range(3):
        index_landed[part, y, z, x] = index[8 * part : 8 * part + 8, :]
    wide = 2 * LANES
    rank = lax.broadcasted_iota(jnp.int32, (wide, wide), 0)
    spot = lax.broadcasted_iota(jnp.int32, (wide, wide), 1)
    wanted = jnp.where(spot < LANES, 2 * spot, 2 * (spot - LANES) + 1)
    split = jnp.where(rank == wanted, 1.0, 0.0).astype(jnp.bfloat16)
    for b, load in enumerate(loads):
        load.wait()
        for n in range(samples // wide):
            at = slice(b * block, (b + 1) * block)
            apart = jnp.dot(held[at, n * wide : (n + 1) * wide], split, preferred_element_type=jnp.float32)
            apart = apart.astype(jnp.bfloat16)
            halves[0, at, n * LANES : (n + 1) * LANES] = apart[:, :LANES]
            halves[1, at, n * LANES : (n + 1) * LANES] = apart[:, LANES:]

    def index_step(stage):
        for part in range(3):
            order = [(2, 1, 0), (1, 0, 2), (0, 2, 1)][part]
            at = [y, z, x]
            for ring in order[:stage]:
                at[ring] = slice(None)
            ref = index_landed.at[(part, *at)]
            for d in range(1, RINGS):
                to = [y, z, x]
                to[order[stage]] = lax.rem(to[order[stage]] + d, RINGS)
                pltpu.make_async_remote_copy(
                    ref, ref, index_sems.at[0, part, stage], index_sems.at[1, part, stage],
                    device_id=(to[0] * 2 + core, to[1] * 4 + to[2]), device_id_type=MESH
                ).start()

    def index_settle(stage, way):
        for part in range(3):
            span = index_landed.at[(part,) + (0,) * (2 - stage) + (pl.ds(0, 3),)]
            pltpu.make_async_copy(span, span, index_sems.at[way, part, stage]).wait()

    def pre_copy(t):
        return pltpu.make_async_remote_copy(
            pre_send.at[t], pre_land.at[t], pre_sems.at[0, t], pre_sems.at[1, t],
            device_id=partner, device_id_type=MESH
        )

    def send_rcv(t):
        q = lax.rem(t + me, RINGS)
        pre_copy(t).wait()
        at = pl.ds(q * PLANE, PLANE)
        rcv_blocks[at] = rcv_blocks[at] + pre_land[t]
        for n in range(PLANE):

            @pl.when(q * PLANE + n != me)
            def _():
                send(rcv_blocks.at[q * PLANE + n], rcv_landed.at[me], 2, (q * 2 + core, n))

    pl.semaphore_wait(barrier, CHIPS)
    index_step(0)

    def chunk_step(t, carry):
        q = lax.rem(t + me, 4)
        fill_tables(table, rows_ref, turns_ref, q)
        first = (lax.broadcasted_iota(jnp.int32, (1, LANES), 1) + q) == 0
        sums = [None, None]
        for b in range(slots // block):
            at = slice(b * block, (b + 1) * block)
            even = jnp.dot(halves[0, at], table[0], preferred_element_type=jnp.float32)
            odd = jnp.dot(halves[1, at], table[1], preferred_element_type=jnp.float32)
            even_c, even_s, odd_c, odd_s = even[:, :LANES], even[:, LANES:], odd[:, :LANES], odd[:, LANES:]
            whole = (even_c + odd_c, jnp.where(first, 0.0, even_s + odd_s))
            mirror = (jnp.where(first, even_s, even_c - odd_c), jnp.where(first, odd_s, even_s - odd_s))
            for n, (real, imag) in enumerate((whole, mirror)):
                logs = jnp.log((real * real + imag * imag) * (1.0 / samples) + 1e-6)
                part = jnp.dot(hot[:, at], two_parts(logs, 1), preferred_element_type=jnp.float32)
                sums[n] = part if b == 0 else sums[n] + part
        for n in range(2):
            total = (sums[n][:, :LANES] + sums[n][:, LANES:]).T
            shot_blocks[pl.ds(q * PLANE + n * 8, 8)] = total[:, :LANES].reshape(8, OWNED, LANES)
            both = total[:, LANES:].reshape(8, 2, OWNED // 2, LANES)
            rcv_blocks[pl.ds(q * PLANE + n * 8, 8)] = jnp.where(core == 0, both[:, 0], both[:, 1])
            pre_send[t, n * 8 : n * 8 + 8] = jnp.where(core == 0, both[:, 1], both[:, 0])

        @pl.when(t == 0)
        def _():
            pass

        for stage in range(1, 3):

            @pl.when(t == stage - 1)
            def _():
                index_settle(stage - 1, 1)
                index_step(stage)

        pre_copy(t).start()
        for n in range(PLANE):

            @pl.when(q * PLANE + n != me)
            def _():
                send(shot_blocks.at[q * PLANE + n], shot_landed.at[me], 1, (q * 2 + core, n))

        @pl.when(t > 0)
        def _():
            send_rcv(t - 1)

        return carry

    lax.fori_loop(0, RINGS, chunk_step, 0)
    shot_landed[me] = shot_blocks[me]

    totals[...] = jnp.zeros_like(totals)

    index_settle(2, 1)

    def pair_step(j, carry):
        across = pl.ds(pl.multiple_of(j * LANES, LANES), LANES)
        count = None
        for b in range(RINGS):
            values = jnp.concatenate([index_landed[part, b, j // 4, lax.rem(j, 4)] for part in range(3)], axis=0)
            values = values.astype(jnp.float32)
            shots = jnp.concatenate([one_hot(values[r : r + 1], ids) for r in range(tiles)], axis=1)
            rcvs = jnp.concatenate([one_hot(values[tiles + r : tiles + r + 1], ids) for r in range(tiles)], axis=1)
            pair = lax.dot_general(shots, rcvs, NT, preferred_element_type=jnp.float32)
            pairs[b * LANES : (b + 1) * LANES, across] = pair.astype(jnp.bfloat16)
            totals[b] += pair
            count = pair if count is None else count + pair
        rcv_count[:, across] = jnp.broadcast_to(count.sum(axis=0, keepdims=True), (8, LANES))
        return carry

    lax.fori_loop(0, 4, pair_step, 0, unroll=2)
    send_rcv(RINGS - 1)
    rcv_landed[me] = rcv_blocks[me]
    lax.fori_loop(4, PLANE, pair_step, 0, unroll=2)

    def pair_copy(src, dst, n):
        return pltpu.make_async_remote_copy(
            src, dst, part_sems.at[0, n], part_sems.at[1, n], device_id=partner, device_id_type=MESH
        )

    count_copy = pair_copy(rcv_count, count_land, SWEEPS)
    count_copy.start()
    counts = jnp.concatenate([totals[b].T.sum(axis=0, keepdims=True) for b in range(RINGS)], axis=1)

    settle(shot_landed, 1, 1)
    settle(rcv_landed, 2, 1)
    shot_logs = jnp.concatenate(
        [shot_landed[b * PLANE : (b + 1) * PLANE].sum(axis=0) for b in range(RINGS)], axis=1
    )
    rcv_logs = rcv_landed[:PLANE]
    for b in range(1, RINGS):
        rcv_logs = rcv_logs + rcv_landed[b * PLANE : (b + 1) * PLANE]
    rcv_logs = jnp.concatenate([rcv_logs[j] for j in range(PLANE)], axis=1)
    rcv_logs = jnp.concatenate(
        [jnp.where(core == 0, rcv_logs, 0.0), jnp.where(core == 0, 0.0, rcv_logs)], axis=0
    )
    count_copy.wait()
    rcv_counts = rcv_count[0:1, :] + count_land[0:1, :]
    copies = [pair_copy(part_send.at[n], part_land.at[n], n) for n in range(SWEEPS)]

    rcv_terms = None
    for n in range(SWEEPS):
        if n == 0:
            shot_terms = shot_logs / counts
        else:
            both = lax.dot_general(two_parts(rcv_terms, 0), pairs[...], NT, preferred_element_type=jnp.float32)
            shot_terms = (shot_logs - (both[:OWNED] + both[OWNED:])) / counts
        if n == SWEEPS - 1:
            for b in range(RINGS):
                shot_send[b] = shot_terms[:, b * LANES : (b + 1) * LANES]
            for ty, _, _, device in away:
                send(shot_send.at[ty], shot_land.at[me], 3, device)
        both = jnp.dot(two_parts(shot_terms, 0), pairs[...], preferred_element_type=jnp.float32)
        part = rcv_logs - (both[:OWNED] + both[OWNED:])
        part_send[n] = part
        copies[n].start()
        copies[n].wait()
        rcv_terms = (part + part_land[n]) / rcv_counts
    own = jnp.where(core == 0, rcv_terms[: OWNED // 2], rcv_terms[OWNED // 2 :])
    for j in range(PLANE):
        rcv_send[j] = own[:, j * LANES : (j + 1) * LANES]
    for _, rcv, _, device in away:
        send(rcv_send.at[rcv], rcv_land.at[core, me], 4, device)
    shot_land[me] = shot_send[y]
    rcv_land[core, me] = rcv_send[mine]
    settle(rcv_land.at[core], 4, 1)
    across = pair_copy(rcv_land.at[core], rcv_land.at[core], SWEEPS + 1)
    across.start()
    settle(shot_land, 3, 1)
    shot_out[...] = shot_land[...]
    for kind, ref in enumerate((shot_landed, rcv_landed, shot_land, rcv_landed)):
        settle(ref, kind + 1, 0)
    for stage in range(3):
        index_settle(stage, 0)
    across.wait()
    rcv_out[...] = rcv_land[...]


def turn_kernel(shot_in, rcv_in, shot_out, rcv_out):
    lane = lax.broadcasted_iota(jnp.int32, (LANES, LANES), 1)
    back = lax.rem(LANES - lane, LANES)
    def chunk(src, n):
        if src.shape[0] == CHIPS:
            bins = src[n * 8 : n * 8 + 8]
        else:
            bins = jnp.stack([src[0, n * 8 : n * 8 + 8], src[1, n * 8 : n * 8 + 8]], axis=1)
        return bins.reshape(LANES, LANES).T

    for src, dst in ((shot_in, shot_out), (rcv_in, rcv_out)):
        mirrors = []
        for q in range(4):
            dst[:, q * LANES : (q + 1) * LANES] = chunk(src, 2 * q)
            mirrors.append(jnp.take_along_axis(chunk(src, 2 * q + 1), back, axis=1))
        for c in range(4, 8):
            head = mirrors[8 - c if c > 4 else 0]
            dst[:, c * LANES : (c + 1) * LANES] = jnp.where(lane == 0, head, mirrors[7 - c])


def shards(traces, trace_shot, trace_rcv, fold_count):
    slots, samples = traces.shape[2:]
    bins = samples // 2
    tiles = slots // LANES
    rows_np, turns_np = phase_tables(samples)
    f32, bf16 = jnp.float32, jnp.bfloat16
    vmem = pl.BlockSpec(memory_space=VMEM)
    shape = jax.ShapeDtypeStruct
    shot_got, rcv_got = pl.pallas_call(
        main_kernel,
        out_shape=(shape((CHIPS, OWNED, LANES), f32), shape((2, CHIPS, OWNED // 2, LANES), f32)),
        in_specs=[pl.BlockSpec(memory_space=pltpu.SMEM), vmem, vmem, pl.BlockSpec(memory_space=pl.ANY), vmem, vmem],
        out_specs=(vmem,) * 2,
        scratch_shapes=[
            VMEM((2 * tiles, LANES), jnp.int32),
            VMEM((slots, samples), bf16),
            VMEM((2, slots, samples // 2), bf16),
            VMEM((2, samples // 2, 2 * LANES), bf16),
            VMEM((2 * LANES, slots), bf16),
            VMEM((CHIPS, OWNED, LANES), f32),
            VMEM((CHIPS, OWNED // 2, LANES), f32),
            VMEM((RINGS, PLANE, OWNED // 2, LANES), f32),
            VMEM((RINGS, PLANE, OWNED // 2, LANES), f32),
            VMEM((CHIPS, OWNED, LANES), f32),
            VMEM((CHIPS, OWNED // 2, LANES), f32),
            VMEM((3, RINGS, RINGS, RINGS, 8, LANES), jnp.int32),
            VMEM((RINGS * LANES, PLANE * LANES), bf16),
            VMEM((RINGS, LANES, LANES), f32),
            VMEM((8, PLANE * LANES), f32),
            VMEM((8, PLANE * LANES), f32),
            VMEM((RINGS, OWNED, LANES), f32),
            VMEM((PLANE, OWNED // 2, LANES), f32),
            VMEM((CHIPS, OWNED, LANES), f32),
            VMEM((2, CHIPS, OWNED // 2, LANES), f32),
            VMEM((SWEEPS, OWNED, PLANE * LANES), f32),
            VMEM((SWEEPS, OWNED, PLANE * LANES), f32),
            pltpu.SemaphoreType.DMA((slots // 512,)),
            pltpu.SemaphoreType.DMA((2, 3, 3)),
            pltpu.SemaphoreType.DMA((2, 5)),
            pltpu.SemaphoreType.DMA((2, RINGS)),
            pltpu.SemaphoreType.DMA((2, SWEEPS + 2)),
        ],
        compiler_params=pltpu.CompilerParams(
            collective_id=0, has_side_effects=True, vmem_limit_bytes=VMEM_LIMIT
        ),
        name="decompose",
    )(fold_count, trace_shot[0], trace_rcv[0], traces[0, 0], jnp.asarray(rows_np), jnp.asarray(turns_np))
    return pl.pallas_call(
        turn_kernel,
        out_shape=(shape((LANES, bins), f32), shape((LANES, bins), f32)),
        in_specs=[vmem] * 2,
        out_specs=(vmem,) * 2,
        compiler_params=pltpu.CompilerParams(vmem_limit_bytes=VMEM_LIMIT),
        name="turn",
    )(shot_got, rcv_got)


def solution(mesh):
    return jax.shard_map(
        shards,
        mesh=mesh,
        in_specs=(
            P("shot", "rcv", None, None),
            P("shot", "rcv", None),
            P("shot", "rcv", None),
            P("shot", "rcv"),
        ),
        out_specs=(P("shot", None), P("rcv", None)),
        check_vma=False,
    )
```

```python
import jax
import jax.numpy as jnp
import numpy as np
from jax import lax
from jax.experimental import pallas as pl
from jax.experimental.pallas import tpu as pltpu
from jax.sharding import PartitionSpec as P

MESH = pl.DeviceIdType.MESH
VMEM = pltpu.VMEM
SWEEPS = 3
LANES = 128
CHIPS = 64
PLANE = 16
RINGS = 4
OWNED = 16
NT = (((1,), (1,)), ((), ()))
VMEM_LIMIT = 50 * 1024 * 1024


def phase_tables(samples):
    lane = np.arange(LANES)
    wave = lambda steps: np.stack([g(2 * np.pi * (steps % samples) / samples) for g in (np.cos, np.sin)])
    rows = wave(16 * lane[:, None] * lane[None, :])
    sub = np.arange(8)[:, None]
    turns = [[wave((2 * sub + odd) * (LANES * q + lane[None, :])) for odd in range(2)] for q in range(4)]
    return rows.astype(np.float32), np.array(turns).astype(np.float32)


def fill_tables(table, rows_ref, turns_ref, q):
    turns = [[turns_ref[q, odd, part] for part in range(2)] for odd in range(2)]

    def step(m, carry):
        tops = [[], []]
        for part in range(2):
            at = 2 * m + part
            rc = jnp.broadcast_to(rows_ref[0, pl.ds(at, 1), :], (8, LANES))
            rs = jnp.broadcast_to(rows_ref[1, pl.ds(at, 1), :], (8, LANES))
            for odd in range(2):
                turn_c, turn_s = turns[odd]
                tops[odd].append(jnp.concatenate([rc * turn_c - rs * turn_s, rs * turn_c + rc * turn_s], axis=1))
        at = pl.ds(pl.multiple_of(m * 16, 16), 16)
        for odd in range(2):
            table[odd, at, :] = jnp.concatenate(tops[odd], axis=0).astype(jnp.bfloat16)
        return carry

    lax.fori_loop(0, 64, step, 0, unroll=8)

    @pl.when(q == 0)
    def _():
        first = lax.broadcasted_iota(jnp.int32, (8, LANES), 1) == 0
        flip = 1.0 - 2.0 * lax.rem(lax.broadcasted_iota(jnp.int32, (8, LANES), 0), 2).astype(jnp.float32)
        flip = jnp.concatenate([flip, flip], axis=0)
        first = jnp.concatenate([first, first], axis=0)
        for odd in range(2):
            for m in range(64):
                at = pl.ds(m * 16, 16)
                old = table[odd, at, LANES:].astype(jnp.float32)
                table[odd, at, LANES:] = jnp.where(first, flip, old).astype(jnp.bfloat16)


def one_hot(row, ids):
    wide = jnp.broadcast_to(row, (16, LANES)).astype(jnp.bfloat16)
    wide = jnp.concatenate([wide] * 8, axis=0)
    return jnp.where(wide == ids, jnp.ones_like(ids), jnp.zeros_like(ids))


def sublane_ids():
    return lax.broadcasted_iota(jnp.int32, (LANES, LANES), 0).astype(jnp.float32).astype(jnp.bfloat16)


def my_place():
    shot, rcv = lax.axis_index("shot"), lax.axis_index("rcv")
    return shot // 2, lax.rem(shot, 2), rcv // 4, lax.rem(rcv, 4)


def others(place):
    y, core, z, x = place
    ys, zs, xs = ([lax.rem(at + d, RINGS) for d in range(RINGS)] for at in (y, z, x))
    found = []
    for k in range(1, CHIPS):
        ty, rcv = ys[k // PLANE], zs[k // 4 % 4] * 4 + xs[k % 4]
        found.append((ty, rcv, ty * PLANE + rcv, (ty * 2 + core, rcv)))
    return found


def two_parts(value, axis):
    top = value.astype(jnp.bfloat16)
    return jnp.concatenate([top, (value - top.astype(jnp.float32)).astype(jnp.bfloat16)], axis=axis)


def main_kernel(fold, trace_shot, trace_rcv, traces, rows_ref, turns_ref, shot_out, rcv_out,
                index, held, halves, table, hot, shot_blocks, rcv_blocks, pre_send, pre_land,
                shot_landed, rcv_landed, index_landed,
                pairs, totals, rcv_count, count_land,
                shot_send, rcv_send, shot_land, rcv_land, part_send, part_land,
                trace_sem, index_sems, sems, pre_sems, part_sems):
    place = my_place()
    y, core, z, x = place
    mine = z * 4 + x
    me = y * PLANE + mine
    partner = (y * 2 + 1 - core, mine)
    slots, samples = held.shape
    tiles = slots // LANES
    away = others(place)

    barrier = pltpu.get_barrier_semaphore()
    for device in [a[3] for a in away] + [partner]:
        pl.semaphore_signal(barrier, inc=1, device_id=device, device_id_type=MESH)

    def send(src, dst, kind, device):
        pltpu.make_async_remote_copy(
            src, dst, sems.at[0, kind], sems.at[1, kind], device_id=device, device_id_type=MESH
        ).start()

    def settle(ref, kind, way):
        span = ref.at[pl.ds(0, CHIPS - 1)]
        pltpu.make_async_copy(span, span, sems.at[way, kind]).wait()

    block = 512
    loads = [
        pltpu.make_async_copy(traces.at[pl.ds(b * block, block)], held.at[pl.ds(b * block, block)], trace_sem.at[b])
        for b in range(slots // block)
    ]
    for load in loads:
        load.start()
    lane = lax.broadcasted_iota(jnp.int32, (1, LANES), 1)
    for r in range(tiles):
        live = lane + r * LANES < fold[0, 0]
        at = slice(r * LANES, (r + 1) * LANES)
        index[r : r + 1, :] = jnp.where(live, trace_shot[:, at], -1)
        index[tiles + r : tiles + r + 1, :] = jnp.where(live, trace_rcv[:, at], -1)
    ids = sublane_ids()
    values = index[...].astype(jnp.float32)
    for r in range(tiles):
        hot[:LANES, r * LANES : (r + 1) * LANES] = one_hot(values[r : r + 1], ids)
        hot[LANES:, r * LANES : (r + 1) * LANES] = one_hot(values[tiles + r : tiles + r + 1], ids)
    for part in range(3):
        index_landed[part, y, z, x] = index[8 * part : 8 * part + 8, :]
    wide = 2 * LANES
    rank = lax.broadcasted_iota(jnp.int32, (wide, wide), 0)
    spot = lax.broadcasted_iota(jnp.int32, (wide, wide), 1)
    wanted = jnp.where(spot < LANES, 2 * spot, 2 * (spot - LANES) + 1)
    split = jnp.where(rank == wanted, 1.0, 0.0).astype(jnp.bfloat16)
    for b, load in enumerate(loads):
        load.wait()
        for n in range(samples // wide):
            at = slice(b * block, (b + 1) * block)
            apart = jnp.dot(held[at, n * wide : (n + 1) * wide], split, preferred_element_type=jnp.float32)
            apart = apart.astype(jnp.bfloat16)
            halves[0, at, n * LANES : (n + 1) * LANES] = apart[:, :LANES]
            halves[1, at, n * LANES : (n + 1) * LANES] = apart[:, LANES:]

    def index_step(stage):
        for part in range(3):
            order = [(2, 1, 0), (1, 0, 2), (0, 2, 1)][part]
            at = [y, z, x]
            for ring in order[:stage]:
                at[ring] = slice(None)
            ref = index_landed.at[(part, *at)]
            for d in range(1, RINGS):
                to = [y, z, x]
                to[order[stage]] = lax.rem(to[order[stage]] + d, RINGS)
                pltpu.make_async_remote_copy(
                    ref, ref, index_sems.at[0, part, stage], index_sems.at[1, part, stage],
                    device_id=(to[0] * 2 + core, to[1] * 4 + to[2]), device_id_type=MESH
                ).start()

    def index_settle(stage, way):
        for part in range(3):
            span = index_landed.at[(part,) + (0,) * (2 - stage) + (pl.ds(0, 3),)]
            pltpu.make_async_copy(span, span, index_sems.at[way, part, stage]).wait()

    def pre_copy(t):
        return pltpu.make_async_remote_copy(
            pre_send.at[t], pre_land.at[t], pre_sems.at[0, t], pre_sems.at[1, t],
            device_id=partner, device_id_type=MESH
        )

    def send_rcv(t):
        q = lax.rem(t + me, RINGS)
        pre_copy(t).wait()
        at = pl.ds(q * PLANE, PLANE)
        rcv_blocks[at] = rcv_blocks[at] + pre_land[t]
        for n in range(PLANE):

            @pl.when(q * PLANE + n != me)
            def _():
                send(rcv_blocks.at[q * PLANE + n], rcv_landed.at[me], 2, (q * 2 + core, n))

    pl.semaphore_wait(barrier, CHIPS)
    index_step(0)

    def chunk_step(t, carry):
        q = lax.rem(t + me, 4)
        fill_tables(table, rows_ref, turns_ref, q)
        first = (lax.broadcasted_iota(jnp.int32, (1, LANES), 1) + q) == 0
        sums = [None, None]
        for b in range(slots // block):
            at = slice(b * block, (b + 1) * block)
            even = jnp.dot(halves[0, at], table[0], preferred_element_type=jnp.float32)
            odd = jnp.dot(halves[1, at], table[1], preferred_element_type=jnp.float32)
            even_c, even_s, odd_c, odd_s = even[:, :LANES], even[:, LANES:], odd[:, :LANES], odd[:, LANES:]
            whole = (even_c + odd_c, jnp.where(first, 0.0, even_s + odd_s))
            mirror = (jnp.where(first, even_s, even_c - odd_c), jnp.where(first, odd_s, even_s - odd_s))
            for n, (real, imag) in enumerate((whole, mirror)):
                logs = jnp.log((real * real + imag * imag) * (1.0 / samples) + 1e-6)
                part = jnp.dot(hot[:, at], two_parts(logs, 1), preferred_element_type=jnp.float32)
                sums[n] = part if b == 0 else sums[n] + part
        for n in range(2):
            total = (sums[n][:, :LANES] + sums[n][:, LANES:]).T
            shot_blocks[pl.ds(q * PLANE + n * 8, 8)] = total[:, :LANES].reshape(8, OWNED, LANES)
            both = total[:, LANES:].reshape(8, 2, OWNED // 2, LANES)
            rcv_blocks[pl.ds(q * PLANE + n * 8, 8)] = jnp.where(core == 0, both[:, 0], both[:, 1])
            pre_send[t, n * 8 : n * 8 + 8] = jnp.where(core == 0, both[:, 1], both[:, 0])

        @pl.when(t == 0)
        def _():
            pass

        for stage in range(1, 3):

            @pl.when(t == stage - 1)
            def _():
                index_settle(stage - 1, 1)
                index_step(stage)

        pre_copy(t).start()
        for n in range(PLANE):

            @pl.when(q * PLANE + n != me)
            def _():
                send(shot_blocks.at[q * PLANE + n], shot_landed.at[me], 1, (q * 2 + core, n))

        @pl.when(t > 0)
        def _():
            send_rcv(t - 1)

        return carry

    lax.fori_loop(0, RINGS, chunk_step, 0)
    shot_landed[me] = shot_blocks[me]

    totals[...] = jnp.zeros_like(totals)

    index_settle(2, 1)

    def pair_step(j, carry):
        across = pl.ds(pl.multiple_of(j * LANES, LANES), LANES)
        count = None
        for b in range(RINGS):
            values = jnp.concatenate([index_landed[part, b, j // 4, lax.rem(j, 4)] for part in range(3)], axis=0)
            values = values.astype(jnp.float32)
            shots = jnp.concatenate([one_hot(values[r : r + 1], ids) for r in range(tiles)], axis=1)
            rcvs = jnp.concatenate([one_hot(values[tiles + r : tiles + r + 1], ids) for r in range(tiles)], axis=1)
            pair = lax.dot_general(shots, rcvs, NT, preferred_element_type=jnp.float32)
            pairs[b * LANES : (b + 1) * LANES, across] = pair.astype(jnp.bfloat16)
            totals[b] += pair
            count = pair if count is None else count + pair
        rcv_count[:, across] = jnp.broadcast_to(count.sum(axis=0, keepdims=True), (8, LANES))
        return carry

    lax.fori_loop(0, 4, pair_step, 0, unroll=2)
    send_rcv(RINGS - 1)
    rcv_landed[me] = rcv_blocks[me]
    lax.fori_loop(4, PLANE, pair_step, 0, unroll=2)

    def pair_copy(src, dst, n):
        return pltpu.make_async_remote_copy(
            src, dst, part_sems.at[0, n], part_sems.at[1, n], device_id=partner, device_id_type=MESH
        )

    count_copy = pair_copy(rcv_count, count_land, SWEEPS)
    count_copy.start()
    counts = jnp.concatenate([totals[b].T.sum(axis=0, keepdims=True) for b in range(RINGS)], axis=1)

    settle(shot_landed, 1, 1)
    settle(rcv_landed, 2, 1)
    shot_logs = jnp.concatenate(
        [shot_landed[b * PLANE : (b + 1) * PLANE].sum(axis=0) for b in range(RINGS)], axis=1
    )
    rcv_logs = rcv_landed[:PLANE]
    for b in range(1, RINGS):
        rcv_logs = rcv_logs + rcv_landed[b * PLANE : (b + 1) * PLANE]
    rcv_logs = jnp.concatenate([rcv_logs[j] for j in range(PLANE)], axis=1)
    rcv_logs = jnp.concatenate(
        [jnp.where(core == 0, rcv_logs, 0.0), jnp.where(core == 0, 0.0, rcv_logs)], axis=0
    )
    count_copy.wait()
    rcv_counts = rcv_count[0:1, :] + count_land[0:1, :]
    copies = [pair_copy(part_send.at[n], part_land.at[n], n) for n in range(SWEEPS)]

    rcv_terms = None
    for n in range(SWEEPS):
        if n == 0:
            shot_terms = shot_logs / counts
        else:
            both = lax.dot_general(two_parts(rcv_terms, 0), pairs[...], NT, preferred_element_type=jnp.float32)
            shot_terms = (shot_logs - (both[:OWNED] + both[OWNED:])) / counts
        if n == SWEEPS - 1:
            for b in range(RINGS):
                shot_send[b] = shot_terms[:, b * LANES : (b + 1) * LANES]
            for ty, _, _, device in away[::-1]:
                send(shot_send.at[ty], shot_land.at[me], 3, device)
        both = jnp.dot(two_parts(shot_terms, 0), pairs[...], preferred_element_type=jnp.float32)
        part = rcv_logs - (both[:OWNED] + both[OWNED:])
        part_send[n] = part
        copies[n].start()
        copies[n].wait()
        rcv_terms = (part + part_land[n]) / rcv_counts
    own = jnp.where(core == 0, rcv_terms[: OWNED // 2], rcv_terms[OWNED // 2 :])
    for j in range(PLANE):
        rcv_send[j] = own[:, j * LANES : (j + 1) * LANES]
    for _, rcv, _, device in away[::-1]:
        send(rcv_send.at[rcv], rcv_land.at[core, me], 4, device)
    shot_land[me] = shot_send[y]
    rcv_land[core, me] = rcv_send[mine]
    settle(rcv_land.at[core], 4, 1)
    across = pair_copy(rcv_land.at[core], rcv_land.at[core], SWEEPS + 1)
    across.start()
    settle(shot_land, 3, 1)
    shot_out[...] = shot_land[...]
    for kind, ref in enumerate((shot_landed, rcv_landed, shot_land, rcv_landed)):
        settle(ref, kind + 1, 0)
    for stage in range(3):
        index_settle(stage, 0)
    across.wait()
    rcv_out[...] = rcv_land[...]


def turn_kernel(shot_in, rcv_in, shot_out, rcv_out):
    lane = lax.broadcasted_iota(jnp.int32, (LANES, LANES), 1)
    back = lax.rem(LANES - lane, LANES)
    def chunk(src, n):
        if src.shape[0] == CHIPS:
            bins = src[n * 8 : n * 8 + 8]
        else:
            bins = jnp.stack([src[0, n * 8 : n * 8 + 8], src[1, n * 8 : n * 8 + 8]], axis=1)
        return bins.reshape(LANES, LANES).T

    for src, dst in ((shot_in, shot_out), (rcv_in, rcv_out)):
        mirrors = []
        for q in range(4):
            dst[:, q * LANES : (q + 1) * LANES] = chunk(src, 2 * q)
            mirrors.append(jnp.take_along_axis(chunk(src, 2 * q + 1), back, axis=1))
        for c in range(4, 8):
            head = mirrors[8 - c if c > 4 else 0]
            dst[:, c * LANES : (c + 1) * LANES] = jnp.where(lane == 0, head, mirrors[7 - c])


def shards(traces, trace_shot, trace_rcv, fold_count):
    slots, samples = traces.shape[2:]
    bins = samples // 2
    tiles = slots // LANES
    rows_np, turns_np = phase_tables(samples)
    f32, bf16 = jnp.float32, jnp.bfloat16
    vmem = pl.BlockSpec(memory_space=VMEM)
    shape = jax.ShapeDtypeStruct
    shot_got, rcv_got = pl.pallas_call(
        main_kernel,
        out_shape=(shape((CHIPS, OWNED, LANES), f32), shape((2, CHIPS, OWNED // 2, LANES), f32)),
        in_specs=[pl.BlockSpec(memory_space=pltpu.SMEM), vmem, vmem, pl.BlockSpec(memory_space=pl.ANY), vmem, vmem],
        out_specs=(vmem,) * 2,
        scratch_shapes=[
            VMEM((2 * tiles, LANES), jnp.int32),
            VMEM((slots, samples), bf16),
            VMEM((2, slots, samples // 2), bf16),
            VMEM((2, samples // 2, 2 * LANES), bf16),
            VMEM((2 * LANES, slots), bf16),
            VMEM((CHIPS, OWNED, LANES), f32),
            VMEM((CHIPS, OWNED // 2, LANES), f32),
            VMEM((RINGS, PLANE, OWNED // 2, LANES), f32),
            VMEM((RINGS, PLANE, OWNED // 2, LANES), f32),
            VMEM((CHIPS, OWNED, LANES), f32),
            VMEM((CHIPS, OWNED // 2, LANES), f32),
            VMEM((3, RINGS, RINGS, RINGS, 8, LANES), jnp.int32),
            VMEM((RINGS * LANES, PLANE * LANES), bf16),
            VMEM((RINGS, LANES, LANES), f32),
            VMEM((8, PLANE * LANES), f32),
            VMEM((8, PLANE * LANES), f32),
            VMEM((RINGS, OWNED, LANES), f32),
            VMEM((PLANE, OWNED // 2, LANES), f32),
            VMEM((CHIPS, OWNED, LANES), f32),
            VMEM((2, CHIPS, OWNED // 2, LANES), f32),
            VMEM((SWEEPS, OWNED, PLANE * LANES), f32),
            VMEM((SWEEPS, OWNED, PLANE * LANES), f32),
            pltpu.SemaphoreType.DMA((slots // 512,)),
            pltpu.SemaphoreType.DMA((2, 3, 3)),
            pltpu.SemaphoreType.DMA((2, 5)),
            pltpu.SemaphoreType.DMA((2, RINGS)),
            pltpu.SemaphoreType.DMA((2, SWEEPS + 2)),
        ],
        compiler_params=pltpu.CompilerParams(
            collective_id=0, has_side_effects=True, vmem_limit_bytes=VMEM_LIMIT
        ),
        name="decompose",
    )(fold_count, trace_shot[0], trace_rcv[0], traces[0, 0], jnp.asarray(rows_np), jnp.asarray(turns_np))
    return pl.pallas_call(
        turn_kernel,
        out_shape=(shape((LANES, bins), f32), shape((LANES, bins), f32)),
        in_specs=[vmem] * 2,
        out_specs=(vmem,) * 2,
        compiler_params=pltpu.CompilerParams(vmem_limit_bytes=8 * 1024 * 1024),
        name="turn",
    )(shot_got, rcv_got)


def solution(mesh):
    return jax.shard_map(
        shards,
        mesh=mesh,
        in_specs=(
            P("shot", "rcv", None, None),
            P("shot", "rcv", None),
            P("shot", "rcv", None),
            P("shot", "rcv"),
        ),
        out_specs=(P("shot", None), P("rcv", None)),
        check_vma=False,
    )
```

```python
import jax
import jax.numpy as jnp
import numpy as np
from jax import lax
from jax.experimental import pallas as pl
from jax.experimental.pallas import tpu as pltpu
from jax.sharding import PartitionSpec as P

MESH = pl.DeviceIdType.MESH
VMEM = pltpu.VMEM
SWEEPS = 3
LANES = 128
CHIPS = 64
PLANE = 16
RINGS = 4
OWNED = 16
NT = (((1,), (1,)), ((), ()))
VMEM_LIMIT = 50 * 1024 * 1024


def phase_tables(samples):
    lane = np.arange(LANES)
    wave = lambda steps: np.stack([g(2 * np.pi * (steps % samples) / samples) for g in (np.cos, np.sin)])
    rows = wave(16 * lane[:, None] * lane[None, :])
    sub = np.arange(8)[:, None]
    turns = [[wave((2 * sub + odd) * (LANES * q + lane[None, :])) for odd in range(2)] for q in range(4)]
    return rows.astype(np.float32), np.array(turns).astype(np.float32)


def fill_tables(table, waves, q):
    turns = [[waves[pl.ds(pl.multiple_of(2 * LANES + (4 * q + 2 * odd + part) * 8, 8), 8), :] for part in range(2)] for odd in range(2)]

    def step(m, carry):
        tops = [[], []]
        for part in range(2):
            at = 2 * m + part
            rc = jnp.broadcast_to(waves[pl.ds(at, 1), :], (8, LANES))
            rs = jnp.broadcast_to(waves[pl.ds(LANES + at, 1), :], (8, LANES))
            for odd in range(2):
                turn_c, turn_s = turns[odd]
                tops[odd].append(jnp.concatenate([rc * turn_c - rs * turn_s, rs * turn_c + rc * turn_s], axis=1))
        at = pl.ds(pl.multiple_of(m * 16, 16), 16)
        for odd in range(2):
            table[odd, at, :] = jnp.concatenate(tops[odd], axis=0).astype(jnp.bfloat16)
        return carry

    lax.fori_loop(0, 64, step, 0, unroll=8)

    @pl.when(q == 0)
    def _():
        first = lax.broadcasted_iota(jnp.int32, (8, LANES), 1) == 0
        flip = 1.0 - 2.0 * lax.rem(lax.broadcasted_iota(jnp.int32, (8, LANES), 0), 2).astype(jnp.float32)
        flip = jnp.concatenate([flip, flip], axis=0)
        first = jnp.concatenate([first, first], axis=0)
        for odd in range(2):
            for m in range(64):
                at = pl.ds(m * 16, 16)
                old = table[odd, at, LANES:].astype(jnp.float32)
                table[odd, at, LANES:] = jnp.where(first, flip, old).astype(jnp.bfloat16)


def one_hot(row, ids):
    wide = jnp.broadcast_to(row, (16, LANES)).astype(jnp.bfloat16)
    wide = jnp.concatenate([wide] * 8, axis=0)
    return jnp.where(wide == ids, jnp.ones_like(ids), jnp.zeros_like(ids))


def sublane_ids():
    return lax.broadcasted_iota(jnp.int32, (LANES, LANES), 0).astype(jnp.float32).astype(jnp.bfloat16)


def my_place():
    shot, rcv = lax.axis_index("shot"), lax.axis_index("rcv")
    return shot // 2, lax.rem(shot, 2), rcv // 4, lax.rem(rcv, 4)


def others(place):
    y, core, z, x = place
    ys, zs, xs = ([lax.rem(at + d, RINGS) for d in range(RINGS)] for at in (y, z, x))
    found = []
    for k in range(1, CHIPS):
        ty, rcv = ys[k // PLANE], zs[k // 4 % 4] * 4 + xs[k % 4]
        found.append((ty, rcv, ty * PLANE + rcv, (ty * 2 + core, rcv)))
    return found


def two_parts(value, axis):
    top = value.astype(jnp.bfloat16)
    return jnp.concatenate([top, (value - top.astype(jnp.float32)).astype(jnp.bfloat16)], axis=axis)


def main_kernel(fold, trace_shot, trace_rcv, traces, waves, shot_out, rcv_out,
                index, held, halves, table, hot, shot_blocks, rcv_blocks, pre_send, pre_land,
                shot_landed, rcv_landed, index_landed,
                pairs, totals, rcv_count, count_land,
                shot_send, rcv_send, shot_land, rcv_land, part_send, part_land,
                trace_sem, index_sems, sems, pre_sems, part_sems):
    place = my_place()
    y, core, z, x = place
    mine = z * 4 + x
    me = y * PLANE + mine
    partner = (y * 2 + 1 - core, mine)
    slots, samples = held.shape
    tiles = slots // LANES
    away = others(place)

    barrier = pltpu.get_barrier_semaphore()
    for device in [a[3] for a in away] + [partner]:
        pl.semaphore_signal(barrier, inc=1, device_id=device, device_id_type=MESH)

    def send(src, dst, kind, device):
        pltpu.make_async_remote_copy(
            src, dst, sems.at[0, kind], sems.at[1, kind], device_id=device, device_id_type=MESH
        ).start()

    def settle(ref, kind, way):
        span = ref.at[pl.ds(0, CHIPS - 1)]
        pltpu.make_async_copy(span, span, sems.at[way, kind]).wait()

    block = 512
    loads = [
        pltpu.make_async_copy(traces.at[pl.ds(b * block, block)], held.at[pl.ds(b * block, block)], trace_sem.at[b])
        for b in range(slots // block)
    ]
    for load in loads:
        load.start()
    lane = lax.broadcasted_iota(jnp.int32, (1, LANES), 1)
    for r in range(tiles):
        live = lane + r * LANES < fold[0, 0]
        at = slice(r * LANES, (r + 1) * LANES)
        index[r : r + 1, :] = jnp.where(live, trace_shot[:, at], -1)
        index[tiles + r : tiles + r + 1, :] = jnp.where(live, trace_rcv[:, at], -1)
    ids = sublane_ids()
    values = index[...].astype(jnp.float32)
    for r in range(tiles):
        hot[:LANES, r * LANES : (r + 1) * LANES] = one_hot(values[r : r + 1], ids)
        hot[LANES:, r * LANES : (r + 1) * LANES] = one_hot(values[tiles + r : tiles + r + 1], ids)
    for part in range(3):
        index_landed[part, y, z, x] = index[8 * part : 8 * part + 8, :]
    wide = 2 * LANES
    rank = lax.broadcasted_iota(jnp.int32, (wide, wide), 0)
    spot = lax.broadcasted_iota(jnp.int32, (wide, wide), 1)
    wanted = jnp.where(spot < LANES, 2 * spot, 2 * (spot - LANES) + 1)
    split = jnp.where(rank == wanted, 1.0, 0.0).astype(jnp.bfloat16)
    for b, load in enumerate(loads):
        load.wait()
        for n in range(samples // wide):
            at = slice(b * block, (b + 1) * block)
            apart = jnp.dot(held[at, n * wide : (n + 1) * wide], split, preferred_element_type=jnp.float32)
            apart = apart.astype(jnp.bfloat16)
            halves[0, at, n * LANES : (n + 1) * LANES] = apart[:, :LANES]
            halves[1, at, n * LANES : (n + 1) * LANES] = apart[:, LANES:]

    def index_step(stage):
        for part in range(3):
            order = [(2, 1, 0), (1, 0, 2), (0, 2, 1)][part]
            at = [y, z, x]
            for ring in order[:stage]:
                at[ring] = slice(None)
            ref = index_landed.at[(part, *at)]
            for d in range(1, RINGS):
                to = [y, z, x]
                to[order[stage]] = lax.rem(to[order[stage]] + d, RINGS)
                pltpu.make_async_remote_copy(
                    ref, ref, index_sems.at[0, part, stage], index_sems.at[1, part, stage],
                    device_id=(to[0] * 2 + core, to[1] * 4 + to[2]), device_id_type=MESH
                ).start()

    def index_settle(stage, way):
        for part in range(3):
            span = index_landed.at[(part,) + (0,) * (2 - stage) + (pl.ds(0, 3),)]
            pltpu.make_async_copy(span, span, index_sems.at[way, part, stage]).wait()

    def pre_copy(t):
        return pltpu.make_async_remote_copy(
            pre_send.at[t], pre_land.at[t], pre_sems.at[0, t], pre_sems.at[1, t],
            device_id=partner, device_id_type=MESH
        )

    def send_rcv(t):
        q = lax.rem(t + me, RINGS)
        pre_copy(t).wait()
        at = pl.ds(q * PLANE, PLANE)
        rcv_blocks[at] = rcv_blocks[at] + pre_land[t]
        for n in range(PLANE):

            @pl.when(q * PLANE + n != me)
            def _():
                send(rcv_blocks.at[q * PLANE + n], rcv_landed.at[me], 2, (q * 2 + core, n))

    pl.semaphore_wait(barrier, CHIPS)
    index_step(0)

    def chunk_step(t, carry):
        q = lax.rem(t + me, 4)
        fill_tables(table, waves, q)
        first = (lax.broadcasted_iota(jnp.int32, (1, LANES), 1) + q) == 0
        sums = [None, None]
        for b in range(slots // block):
            at = slice(b * block, (b + 1) * block)
            even = jnp.dot(halves[0, at], table[0], preferred_element_type=jnp.float32)
            odd = jnp.dot(halves[1, at], table[1], preferred_element_type=jnp.float32)
            even_c, even_s, odd_c, odd_s = even[:, :LANES], even[:, LANES:], odd[:, :LANES], odd[:, LANES:]
            whole = (even_c + odd_c, jnp.where(first, 0.0, even_s + odd_s))
            mirror = (jnp.where(first, even_s, even_c - odd_c), jnp.where(first, odd_s, even_s - odd_s))
            for n, (real, imag) in enumerate((whole, mirror)):
                logs = jnp.log((real * real + imag * imag) * (1.0 / samples) + 1e-6)
                part = jnp.dot(hot[:, at], two_parts(logs, 1), preferred_element_type=jnp.float32)
                sums[n] = part if b == 0 else sums[n] + part
        for n in range(2):
            total = (sums[n][:, :LANES] + sums[n][:, LANES:]).T
            shot_blocks[pl.ds(q * PLANE + n * 8, 8)] = total[:, :LANES].reshape(8, OWNED, LANES)
            both = total[:, LANES:].reshape(8, 2, OWNED // 2, LANES)
            rcv_blocks[pl.ds(q * PLANE + n * 8, 8)] = jnp.where(core == 0, both[:, 0], both[:, 1])
            pre_send[t, n * 8 : n * 8 + 8] = jnp.where(core == 0, both[:, 1], both[:, 0])

        @pl.when(t == 0)
        def _():
            pass

        for stage in range(1, 3):

            @pl.when(t == stage - 1)
            def _():
                index_settle(stage - 1, 1)
                index_step(stage)

        pre_copy(t).start()
        for n in range(PLANE):

            @pl.when(q * PLANE + n != me)
            def _():
                send(shot_blocks.at[q * PLANE + n], shot_landed.at[me], 1, (q * 2 + core, n))

        @pl.when(t > 0)
        def _():
            send_rcv(t - 1)

        return carry

    lax.fori_loop(0, RINGS, chunk_step, 0)
    shot_landed[me] = shot_blocks[me]

    totals[...] = jnp.zeros_like(totals)

    index_settle(2, 1)

    def pair_step(j, carry):
        across = pl.ds(pl.multiple_of(j * LANES, LANES), LANES)
        count = None
        for b in range(RINGS):
            values = jnp.concatenate([index_landed[part, b, j // 4, lax.rem(j, 4)] for part in range(3)], axis=0)
            values = values.astype(jnp.float32)
            shots = jnp.concatenate([one_hot(values[r : r + 1], ids) for r in range(tiles)], axis=1)
            rcvs = jnp.concatenate([one_hot(values[tiles + r : tiles + r + 1], ids) for r in range(tiles)], axis=1)
            pair = lax.dot_general(shots, rcvs, NT, preferred_element_type=jnp.float32)
            pairs[b * LANES : (b + 1) * LANES, across] = pair.astype(jnp.bfloat16)
            totals[b] += pair
            count = pair if count is None else count + pair
        rcv_count[:, across] = jnp.broadcast_to(count.sum(axis=0, keepdims=True), (8, LANES))
        return carry

    lax.fori_loop(0, 4, pair_step, 0, unroll=2)
    send_rcv(RINGS - 1)
    rcv_landed[me] = rcv_blocks[me]
    lax.fori_loop(4, PLANE, pair_step, 0, unroll=2)

    def pair_copy(src, dst, n):
        return pltpu.make_async_remote_copy(
            src, dst, part_sems.at[0, n], part_sems.at[1, n], device_id=partner, device_id_type=MESH
        )

    count_copy = pair_copy(rcv_count, count_land, SWEEPS)
    count_copy.start()
    counts = jnp.concatenate([totals[b].T.sum(axis=0, keepdims=True) for b in range(RINGS)], axis=1)

    settle(shot_landed, 1, 1)
    settle(rcv_landed, 2, 1)
    shot_logs = jnp.concatenate(
        [shot_landed[b * PLANE : (b + 1) * PLANE].sum(axis=0) for b in range(RINGS)], axis=1
    )
    rcv_logs = rcv_landed[:PLANE]
    for b in range(1, RINGS):
        rcv_logs = rcv_logs + rcv_landed[b * PLANE : (b + 1) * PLANE]
    rcv_logs = jnp.concatenate([rcv_logs[j] for j in range(PLANE)], axis=1)
    rcv_logs = jnp.concatenate(
        [jnp.where(core == 0, rcv_logs, 0.0), jnp.where(core == 0, 0.0, rcv_logs)], axis=0
    )
    count_copy.wait()
    rcv_counts = rcv_count[0:1, :] + count_land[0:1, :]
    copies = [pair_copy(part_send.at[n], part_land.at[n], n) for n in range(SWEEPS)]

    rcv_terms = None
    for n in range(SWEEPS):
        if n == 0:
            shot_terms = shot_logs / counts
        else:
            both = lax.dot_general(two_parts(rcv_terms, 0), pairs[...], NT, preferred_element_type=jnp.float32)
            shot_terms = (shot_logs - (both[:OWNED] + both[OWNED:])) / counts
        if n == SWEEPS - 1:
            for b in range(RINGS):
                shot_send[b] = shot_terms[:, b * LANES : (b + 1) * LANES]
            for ty, _, _, device in away[::-1]:
                send(shot_send.at[ty], shot_land.at[me], 3, device)
        both = jnp.dot(two_parts(shot_terms, 0), pairs[...], preferred_element_type=jnp.float32)
        part = rcv_logs - (both[:OWNED] + both[OWNED:])
        part_send[n] = part
        copies[n].start()
        copies[n].wait()
        rcv_terms = (part + part_land[n]) / rcv_counts
    own = jnp.where(core == 0, rcv_terms[: OWNED // 2], rcv_terms[OWNED // 2 :])
    for j in range(PLANE):
        rcv_send[j] = own[:, j * LANES : (j + 1) * LANES]
    for _, rcv, _, device in away[::-1]:
        send(rcv_send.at[rcv], rcv_land.at[core, me], 4, device)
    shot_land[me] = shot_send[y]
    rcv_land[core, me] = rcv_send[mine]
    settle(rcv_land.at[core], 4, 1)
    across = pair_copy(rcv_land.at[core], rcv_land.at[core], SWEEPS + 1)
    across.start()
    settle(shot_land, 3, 1)
    shot_out[...] = shot_land[...]
    for kind, ref in enumerate((shot_landed, rcv_landed, shot_land, rcv_landed)):
        settle(ref, kind + 1, 0)
    for stage in range(3):
        index_settle(stage, 0)
    across.wait()
    rcv_out[...] = rcv_land[...]


def turn_kernel(shot_in, rcv_in, shot_out, rcv_out):
    lane = lax.broadcasted_iota(jnp.int32, (LANES, LANES), 1)
    back = lax.rem(LANES - lane, LANES)
    def chunk(src, n):
        if src.shape[0] == CHIPS:
            bins = src[n * 8 : n * 8 + 8]
        else:
            bins = jnp.stack([src[0, n * 8 : n * 8 + 8], src[1, n * 8 : n * 8 + 8]], axis=1)
        return bins.reshape(LANES, LANES).T

    for src, dst in ((shot_in, shot_out), (rcv_in, rcv_out)):
        mirrors = []
        for q in range(4):
            dst[:, q * LANES : (q + 1) * LANES] = chunk(src, 2 * q)
            mirrors.append(jnp.take_along_axis(chunk(src, 2 * q + 1), back, axis=1))
        for c in range(4, 8):
            head = mirrors[8 - c if c > 4 else 0]
            dst[:, c * LANES : (c + 1) * LANES] = jnp.where(lane == 0, head, mirrors[7 - c])


def shards(traces, trace_shot, trace_rcv, fold_count):
    slots, samples = traces.shape[2:]
    bins = samples // 2
    tiles = slots // LANES
    rows_np, turns_np = phase_tables(samples)
    f32, bf16 = jnp.float32, jnp.bfloat16
    vmem = pl.BlockSpec(memory_space=VMEM)
    shape = jax.ShapeDtypeStruct
    shot_got, rcv_got = pl.pallas_call(
        main_kernel,
        out_shape=(shape((CHIPS, OWNED, LANES), f32), shape((2, CHIPS, OWNED // 2, LANES), f32)),
        in_specs=[pl.BlockSpec(memory_space=pltpu.SMEM), vmem, vmem, pl.BlockSpec(memory_space=pl.ANY), vmem],
        out_specs=(vmem,) * 2,
        scratch_shapes=[
            VMEM((2 * tiles, LANES), jnp.int32),
            VMEM((slots, samples), bf16),
            VMEM((2, slots, samples // 2), bf16),
            VMEM((2, samples // 2, 2 * LANES), bf16),
            VMEM((2 * LANES, slots), bf16),
            VMEM((CHIPS, OWNED, LANES), f32),
            VMEM((CHIPS, OWNED // 2, LANES), f32),
            VMEM((RINGS, PLANE, OWNED // 2, LANES), f32),
            VMEM((RINGS, PLANE, OWNED // 2, LANES), f32),
            VMEM((CHIPS, OWNED, LANES), f32),
            VMEM((CHIPS, OWNED // 2, LANES), f32),
            VMEM((3, RINGS, RINGS, RINGS, 8, LANES), jnp.int32),
            VMEM((RINGS * LANES, PLANE * LANES), bf16),
            VMEM((RINGS, LANES, LANES), f32),
            VMEM((8, PLANE * LANES), f32),
            VMEM((8, PLANE * LANES), f32),
            VMEM((RINGS, OWNED, LANES), f32),
            VMEM((PLANE, OWNED // 2, LANES), f32),
            VMEM((CHIPS, OWNED, LANES), f32),
            VMEM((2, CHIPS, OWNED // 2, LANES), f32),
            VMEM((SWEEPS, OWNED, PLANE * LANES), f32),
            VMEM((SWEEPS, OWNED, PLANE * LANES), f32),
            pltpu.SemaphoreType.DMA((slots // 512,)),
            pltpu.SemaphoreType.DMA((2, 3, 3)),
            pltpu.SemaphoreType.DMA((2, 5)),
            pltpu.SemaphoreType.DMA((2, RINGS)),
            pltpu.SemaphoreType.DMA((2, SWEEPS + 2)),
        ],
        compiler_params=pltpu.CompilerParams(
            collective_id=0, has_side_effects=True, vmem_limit_bytes=VMEM_LIMIT
        ),
        name="decompose",
    )(fold_count, trace_shot[0], trace_rcv[0], traces[0, 0], jnp.asarray(np.concatenate([rows_np.reshape(-1, LANES), turns_np.reshape(-1, LANES)])))
    return pl.pallas_call(
        turn_kernel,
        out_shape=(shape((LANES, bins), f32), shape((LANES, bins), f32)),
        in_specs=[vmem] * 2,
        out_specs=(vmem,) * 2,
        compiler_params=pltpu.CompilerParams(vmem_limit_bytes=8 * 1024 * 1024),
        name="turn",
    )(shot_got, rcv_got)


def solution(mesh):
    return jax.shard_map(
        shards,
        mesh=mesh,
        in_specs=(
            P("shot", "rcv", None, None),
            P("shot", "rcv", None),
            P("shot", "rcv", None),
            P("shot", "rcv"),
        ),
        out_specs=(P("shot", None), P("rcv", None)),
        check_vma=False,
    )
```
